32 devices in a mesh: seg: 4 (over y, x), lat: 8 (over z, core).
Axes of the slice: x: 2, y: 2, z: 4, core: 2. Of those that a mesh axis runs over, the one named last changes fastest.
Arguments:
- coh_map: bfloat16 [4, 65536, 128], P('seg', 'lat'), may hold values from 0 to 40, as said below
- positions: int32 [4, 1024], P('seg', 'lat'), may hold values from 0 to 16776959, as said below
- counts: int32 [16], P('lat'), may hold values from 1 to 64, as said below
Outputs:
- semi_stat: bfloat16 [1024, 128], P('lat')
- excess: float32 [16, 128], P('lat')
The draws below stay inside these ranges and needn't reach their ends.
Inputs may be any that keep to these rules, and one draw needn't show every extreme that they name: `coh_map`: nonnegative. `counts`: the first block has 1 valid point and the last block 64. `positions`: the bins are split into 8 aligned slices of 8192 bins; a point's two bins lie in the same slice; in each segment, at most 32 of the 128 points of one index of lat have their bins in one slice, and that most is reached in every draw.
All inputs are finite; a program needn't handle non-finite values.
Results may differ from the reference program's by a relative error of at most 0.001.
Values sent between devices are 32-bit elements; how exact they have to be, the bound alone decides.
A program may use at most 64 MiB of HBM per device.

```python
import math
import jax
import jax.numpy as jnp
from jax import lax

F = 65536
NSD = 128
BLK = 64
PT_DEV = 128
S = 4
NB = 16
SLICE = 8192
N_LAT = 8


def draw_coh_map(key, part):
    first_key, second_key, third_key = jax.random.split(jax.random.fold_in(key, 11), 3)
    column_scale = jnp.exp(jax.random.uniform(third_key, (NSD,), jnp.float32, math.log(0.1), 0.0))
    values = 2.0 * (jax.random.exponential(first_key, (S, F, NSD), jnp.float32) + jax.random.exponential(second_key, (S, F, NSD), jnp.float32))
    return jnp.clip(values * column_scale, 0.0, 40.0).astype(jnp.bfloat16)


def draw_positions(key, part):
    base_key = jax.random.fold_in(key, 37)
    perm_key, split_key, shuffle_key, bin_key, frac_key = jax.random.split(base_key, 5)
    pair_total = N_LAT // 2
    slot_limit = 2 * PT_DEV // N_LAT
    dest_scores = jax.random.randint(perm_key, (S, N_LAT, N_LAT), 0, 1 << 20, dtype=jnp.int32) * N_LAT + jnp.arange(N_LAT, dtype=jnp.int32)
    dest_perm = jnp.argsort(dest_scores, axis=-1, stable=True).astype(jnp.int32)
    split_at = jax.random.randint(split_key, (S, N_LAT, pair_total), 0, slot_limit + 1, dtype=jnp.int32)
    split_at = split_at.at[:, :, 0].set(slot_limit)
    point_ids = jnp.arange(PT_DEV, dtype=jnp.int32)
    pair_ids = point_ids // slot_limit
    within = point_ids % slot_limit
    split_points = jnp.take(split_at, pair_ids, axis=2)
    first_dest = jnp.take(dest_perm, 2 * pair_ids, axis=2)
    second_dest = jnp.take(dest_perm, 2 * pair_ids + 1, axis=2)
    dest = jnp.where(within[None, None, :] < split_points, first_dest, second_dest)
    point_scores = jax.random.randint(shuffle_key, (S, N_LAT, PT_DEV), 0, 1 << 20, dtype=jnp.int32) * PT_DEV + point_ids
    shuffle = jnp.argsort(point_scores, axis=-1, stable=True).astype(jnp.int32)
    dest = jnp.take_along_axis(dest, shuffle, axis=-1)
    low_bin = dest * SLICE + jax.random.randint(bin_key, (S, N_LAT, PT_DEV), 0, SLICE - 1, dtype=jnp.int32)
    drawn = low_bin * 256 + jax.random.randint(frac_key, (S, N_LAT, PT_DEV), 0, 256, dtype=jnp.int32)
    return drawn.reshape(S, N_LAT * PT_DEV).astype(jnp.int32)


def draw_counts(key, part):
    block_id = jnp.arange(NB, dtype=jnp.int32)
    low_bound = 1 + BLK // 2 * block_id // NB
    high_bound = 1 + BLK // 4 + 3 * BLK // 4 * block_id // NB
    raw_bits = jax.random.randint(jax.random.fold_in(key, 23), (NB,), 0, 1 << 20, dtype=jnp.int32)
    drawn = low_bound + raw_bits % (high_bound - low_bound)
    drawn = drawn.at[0].set(1).at[NB - 1].set(BLK)
    return drawn.astype(jnp.int32)


def setup_inputs(seed: int = 0) -> dict:
    key_list = jax.random.split(jax.random.key(seed), 4)
    coh_map = draw_coh_map(jax.random.fold_in(key_list[3], 71), 0)
    positions = draw_positions(jax.random.fold_in(key_list[3], 71), 0)
    counts = draw_counts(jax.random.fold_in(key_list[3], 71), 0)
    return {"coh_map": coh_map, "positions": positions, "counts": counts}


def reference(coh_map, positions, counts):
    low_bin = positions // 256
    fraction = (positions % 256).astype(jnp.float32) / 256.0

    def accumulate(running, inputs):
        seg_map, low_index, weight_hi = inputs
        near_rows = jnp.take(seg_map, low_index, axis=0).astype(jnp.float32)
        far_rows = jnp.take(seg_map, low_index + 1, axis=0).astype(jnp.float32)
        running = running + (1.0 - weight_hi)[:, None] * near_rows + weight_hi[:, None] * far_rows
        return running, None

    start_sum = jnp.zeros((positions.shape[1], coh_map.shape[2]), jnp.float32)
    summed, _ = lax.scan(accumulate, start_sum, (coh_map, low_bin, fraction))
    semi_stat = summed / coh_map.shape[0]
    grouped = semi_stat.reshape(NB, BLK, NSD)
    slot_index = lax.broadcasted_iota(jnp.int32, (NB, BLK, 1), 1)
    live_mask = slot_index < counts[:, None, None]
    block_sum = jnp.sum(jnp.where(live_mask, grouped, 0.0), axis=1)
    count_float = counts.astype(jnp.float32)
    block_mean = block_sum / count_float[:, None]
    global_mean = jnp.sum(block_sum, axis=0) / jnp.sum(count_float)
    excess = block_mean - global_mean[None, :]
    return semi_stat.astype(jnp.bfloat16), excess
```

```python
import functools

import jax
import jax.numpy as jnp
from jax import lax
from jax.experimental import pallas as pl
from jax.experimental.pallas import tpu as pltpu
from jax.sharding import PartitionSpec as P

MESH = pl.DeviceIdType.MESH
PARTS = 4


def flip(index, mask):
    out = index
    w = 1
    while w <= mask:
        if mask & w:
            out = out + w - 2 * w * lax.rem(index // w, 2)
        w *= 2
    return out


def kernel(
    n_lat,
    n_seg,
    pos_hbm,
    cnt_hbm,
    coh_hbm,
    semi_ref,
    excess_ref,
    pos_ref,
    cnt_ref,
    coh,
    gath,
    rows_out,
    rows_in,
    col_out,
    col_in,
    sid_in,
    far_rows,
    psum,
    psum_in,
    coh_sem,
    gs_sem,
    gr_sem,
    rs_sem,
    rr_sem,
    cs_sem,
    cr_sem,
    xs_sem,
    xr_sem,
    ss_sem,
    sr_sem,
    ps_sem,
    pr_sem,
    in_sem,
):
    lat = lax.axis_index("lat")
    seg = lax.axis_index("seg")
    slice_bins, width = coh.shape
    points = pos_ref.shape[1]
    blocks = cnt_ref.shape[0]
    block_size = points // blocks
    slots = 2 * points // n_lat
    total_slots = n_lat * slots
    f32, bf16, i32 = jnp.float32, jnp.bfloat16, jnp.int32
    group = n_lat // PARTS
    span = group * slots
    quarter = lat // group

    def remote(src, dst, send_sem, recv_sem, to):
        return pltpu.make_async_remote_copy(
            src_ref=src,
            dst_ref=dst,
            send_sem=send_sem,
            recv_sem=recv_sem,
            device_id=to,
            device_id_type=MESH,
        )

    barrier = pltpu.get_barrier_semaphore()
    lat_peers = [flip(lat, j) for j in range(n_lat)]
    seg_peers = [flip(seg, m) for m in range(n_seg)]
    far_first = list(range(n_lat - 1, 0, -1))
    seg_far_first = list(range(n_seg - 1, 0, -1))
    for j in far_first:
        pl.semaphore_signal(barrier, inc=1, device_id=(seg, lat_peers[j]), device_id_type=MESH)
    for m in seg_far_first:
        pl.semaphore_signal(barrier, inc=1, device_id=(seg_peers[m], lat), device_id_type=MESH)

    small = [
        pltpu.make_async_copy(pos_hbm, pos_ref, in_sem.at[0]),
        pltpu.make_async_copy(cnt_hbm, cnt_ref, in_sem.at[1]),
    ]
    for copy in small:
        copy.start()
    load = pltpu.make_async_copy(coh_hbm.at[0], coh, coh_sem)
    load.start()
    for copy in small:
        copy.wait()

    pos = pos_ref[...]
    lane = lax.broadcasted_iota(i32, (1, points), 1)
    dest = (pos // 256) // slice_bins
    rel = jnp.bitwise_xor(dest, jnp.full((1, points), lat, i32))
    hits = lax.broadcasted_iota(i32, (n_lat, points), 0) == rel
    hits_f = hits.astype(f32)
    tri = (
        lax.broadcasted_iota(i32, (points, points), 0)
        < lax.broadcasted_iota(i32, (points, points), 1)
    ).astype(f32)
    before = jnp.dot(hits_f.astype(bf16), tri.astype(bf16), preferred_element_type=f32)
    slot = jnp.sum(before * hits_f, axis=0, keepdims=True).astype(i32)
    sid = rel * slots + slot
    limit = jnp.zeros((1, points), i32)
    for b in range(blocks):
        limit = jnp.where(lane // block_size == b, cnt_ref[b], limit)
    valid = (lane % block_size < limit).astype(i32)
    gath[0, 0:1, :] = sid
    gath[0, 1:2, :] = pos
    gath[0, 2:3, :] = valid
    gath[0, 3:4, :] = valid
    pl.semaphore_wait(barrier, n_lat - 1 + n_seg - 1)

    sends = {
        j: remote(gath.at[0], gath.at[j], gs_sem, gr_sem.at[j // group], (seg, lat_peers[j]))
        for j in far_first
    }
    for j in far_first:
        sends[j].start()
    sid_sends = [
        remote(gath.at[0], sid_in.at[m], ss_sem, sr_sem, (seg_peers[m], lat))
        for m in seg_far_first
    ]
    for copy in sid_sends:
        copy.start()

    pos_bits = 8
    bin_bits = (slice_bins - 1).bit_length()
    depth = min(256, slice_bins)
    depth_bits = depth.bit_length() - 1
    base = lat * (slice_bins << pos_bits)
    flag = slice_bins << pos_bits
    sub = lax.broadcasted_iota(i32, (slots, points), 0)
    bins = lax.broadcasted_iota(i32, (span, depth), 1)
    zero = jnp.zeros((span, depth), bf16)
    chunks = slice_bins // depth
    count = jnp.zeros((1, points), i32)
    col = jnp.zeros((1, width), f32)
    swap = quarter // 3

    def order(part_id):
        first, peers = part_id * group, lat_peers[part_id * group : (part_id + 1) * group]
        if part_id >= 2:
            other = 5 - part_id
            first = first + swap * (other - part_id) * group
            peers = [
                near + swap * (lat_peers[other * group + i] - near) for i, near in enumerate(peers)
            ]
        return first, peers

    def hand_on(src, j, g):
        for m in seg_far_first:
            copy = remote(
                src, far_rows.at[m, j], xs_sem, xr_sem.at[g], (seg_peers[m], lat)
            )
            copy.start()

    for part_id in range(PARTS):
        first, peers = order(part_id)
        rng = pl.ds(first, group) if part_id else pl.ds(1, group - 1)
        remote(gath.at[rng], gath.at[rng], gs_sem, gr_sem.at[first // group], (seg, peers[-1])).wait_recv()
        cols = []
        for i in range(group):
            j = first + i
            live_row = gath[j, 2:3, :]
            code = (gath[j, 1:2, :] - base + flag * (1 + live_row)).astype(f32)
            here = (gath[j, 0:1, :] - j * slots) == sub
            cols.append(jnp.sum(jnp.where(here, code, 0.0), axis=1, keepdims=True))
            count = count + live_row
        code = jnp.concatenate(cols, axis=0).astype(i32)
        kind = lax.shift_right_logical(code, bin_bits + pos_bits)
        low = lax.shift_right_logical(code & (flag - 1), pos_bits)
        upper = (code & ((1 << pos_bits) - 1)).astype(f32) * (1.0 / (1 << pos_bits))
        chunk = jnp.where(kind > 0, lax.shift_right_logical(low, depth_bits), -2)
        in_chunk = low & (depth - 1)
        local = jnp.where(bins == in_chunk, 1.0 - upper, 0.0)
        local = jnp.where(bins == ((in_chunk + 1) & (depth - 1)), upper, local).astype(bf16)
        where_id = jnp.where(bins < in_chunk, chunk + 1, chunk).astype(f32).astype(bf16)
        if part_id == 0:
            load.wait()
        weights = jnp.concatenate(
            [jnp.where(where_id == jnp.asarray(c, bf16), local, zero) for c in range(chunks)],
            axis=1,
        )
        held = jnp.dot(weights, coh[...], preferred_element_type=f32)
        for i in range(group):
            rows_out[first + i] = held[i * slots : (i + 1) * slots, :]
        col = col + jnp.sum(jnp.where(kind > 1, held, 0.0), axis=0, keepdims=True)
        for i in reversed(range(group)):
            if part_id == 0 and i == 0:
                continue
            j = first + i
            copy = remote(
                rows_out.at[j], rows_in.at[j], rs_sem, rr_sem.at[j], (seg, peers[i])
            )
            copy.start()
        if part_id == 0:
            hand_on(rows_out.at[0], 0, 0)
    col_out[0] = col
    for j in far_first:
        remote(col_out.at[0], col_in.at[j], cs_sem, cr_sem, (seg, lat_peers[j])).start()
    total_count = jnp.sum(count.astype(f32), axis=1, keepdims=True)

    for part_id in range(PARTS):
        first, peers = order(part_id)
        for i in range(group):
            j = first + i
            if part_id or i:
                remote(
                    rows_out.at[j], rows_in.at[j], rs_sem, rr_sem.at[j], (seg, peers[i])
                ).wait_recv()
                hand_on(rows_in.at[j], j, first // group)

    def tree(terms):
        w = 1
        while w < n_seg:
            terms = [terms[i] + terms[i + 1] for i in range(0, len(terms), 2)]
            w *= 2
        return terms[0]

    rng = pl.ds(1, n_lat - 1)
    seg_rng = pl.ds(1, n_seg - 1)
    cols = remote(col_in.at[rng], col_in.at[rng], cs_sem, cr_sem, (seg, lat_peers[1]))
    cols.wait_recv()
    for j in range(1, n_lat):
        col = col + col_in[j]
    psum[0] = col
    for m in seg_far_first:
        remote(psum.at[0], psum_in.at[m], ps_sem, pr_sem, (seg_peers[m], lat)).start()
    psums = remote(psum_in.at[seg_rng], psum_in.at[seg_rng], ps_sem, pr_sem, (seg_peers[1], lat))

    sids = remote(sid_in.at[seg_rng], sid_in.at[seg_rng], ss_sem, sr_sem, (seg_peers[1], lat))
    sids.wait_recv()
    slot_row = lax.broadcasted_iota(i32, (total_slots, points), 0)
    picks = []
    for m in range(n_seg):
        theirs = sid_in[m, 0:1, :] if m else sid
        picks.append((slot_row == theirs).astype(f32).T.astype(bf16))
    remote(gath.at[rng], gath.at[rng], gs_sem, gr_sem.at[0], (seg, lat_peers[1])).wait_send()
    remote(rows_out.at[rng], rows_in.at[rng], rs_sem, rr_sem.at[0], (seg, lat_peers[1])).wait_send()
    cols.wait_send()
    sids.wait_send()

    total = jnp.zeros((points, width), f32)
    for part_id in range(PARTS):
        first = part_id * group
        theirs = far_rows.at[seg_rng, pl.ds(first, group)]
        remote(theirs, theirs, xs_sem, xr_sem.at[part_id], (seg_peers[1], lat)).wait_recv()
        got = []
        mine = []
        for m in range(n_seg):
            mine.append(picks[m][:, first * slots : (first + group) * slots])
            for j in range(first, first + group):
                if m:
                    got.append(far_rows[m, j])
                else:
                    got.append(rows_in[j] if j else rows_out[0])
        got = jnp.concatenate(got, axis=0)
        high = got.astype(bf16)
        rest = (got - high.astype(f32)).astype(bf16)
        total = total + jnp.dot(
            jnp.concatenate(mine + mine, axis=1),
            jnp.concatenate([high, rest], axis=0),
            preferred_element_type=f32,
        )
    stat = total / n_seg
    semi_ref[...] = stat.astype(semi_ref.dtype)
    psums.wait_recv()
    col = tree([col] + [psum_in[m] for m in range(1, n_seg)])
    global_mean = (col / n_seg) / total_count
    row = lax.broadcasted_iota(i32, (block_size, width), 0)
    for b in range(blocks):
        block = stat[b * block_size : (b + 1) * block_size]
        block_sum = jnp.sum(jnp.where(row < cnt_ref[b], block, 0.0), axis=0, keepdims=True)
        mean = block_sum / jnp.full((1, width), cnt_ref[b], i32).astype(f32)
        excess_ref[b : b + 1, :] = mean - global_mean

    psums.wait_send()
    theirs = far_rows.at[seg_rng]
    remote(theirs, theirs, xs_sem, xr_sem.at[0], (seg_peers[1], lat)).wait_send()


def deliver(semi_ref, excess_ref, semi_out, excess_out, sem):
    copies = [
        pltpu.make_async_copy(semi_ref, semi_out, sem.at[0]),
        pltpu.make_async_copy(excess_ref, excess_out, sem.at[1]),
    ]
    for copy in copies:
        copy.start()
    for copy in copies:
        copy.wait()


def shards(n_lat, n_seg, coh_map, positions, counts):
    _, slice_bins, width = coh_map.shape
    points = positions.shape[1]
    blocks = counts.shape[0]
    slots = 2 * points // n_lat
    f32 = jnp.float32
    dma = pltpu.SemaphoreType.DMA
    made = pl.pallas_call(
        functools.partial(kernel, n_lat, n_seg),
        out_shape=(
            pltpu.VMEM((points, width), jnp.bfloat16),
            pltpu.VMEM((blocks, width), f32),
        ),
        in_specs=[
            pl.BlockSpec(memory_space=pl.ANY),
            pl.BlockSpec(memory_space=pl.ANY),
            pl.BlockSpec(memory_space=pl.ANY),
        ],
        out_specs=(
            pl.BlockSpec(memory_space=pltpu.VMEM),
            pl.BlockSpec(memory_space=pltpu.VMEM),
        ),
        scratch_shapes=[
            pltpu.VMEM((1, points), jnp.int32),
            pltpu.SMEM((blocks,), jnp.int32),
            pltpu.VMEM((slice_bins, width), coh_map.dtype),
            pltpu.VMEM((n_lat, 4, points), jnp.int32),
            pltpu.VMEM((n_lat, slots, width), f32),
            pltpu.VMEM((n_lat, slots, width), f32),
            pltpu.VMEM((1, 1, width), f32),
            pltpu.VMEM((n_lat, 1, width), f32),
            pltpu.VMEM((n_seg, 4, points), jnp.int32),
            pltpu.VMEM((n_seg, n_lat, slots, width), f32),
            pltpu.VMEM((1, 1, width), f32),
            pltpu.VMEM((n_seg, 1, width), f32),
            dma,
            dma,
            dma((PARTS,)),
            dma,
            dma((n_lat,)),
            dma,
            dma,
            dma,
            dma((PARTS,)),
            dma,
            dma,
            dma,
            dma,
            dma((2,)),
        ],
        compiler_params=pltpu.CompilerParams(collective_id=0, has_side_effects=True),
    )(positions, counts, coh_map)
    made = [pltpu.with_memory_space_constraint(x, pltpu.VMEM) for x in made]
    return pl.pallas_call(
        deliver,
        out_shape=tuple(jax.ShapeDtypeStruct(x.shape, x.dtype) for x in made),
        in_specs=[pl.BlockSpec(memory_space=pltpu.VMEM)] * 2,
        out_specs=(pl.BlockSpec(memory_space=pl.ANY),) * 2,
        scratch_shapes=[dma((2,))],
    )(*made)


def solution(mesh):
    in_specs = (P("seg", "lat", None), P("seg", "lat"), P("lat"))
    out_specs = (P("lat", None), P("lat", None))
    body = functools.partial(shards, mesh.shape["lat"], mesh.shape["seg"])
    return jax.shard_map(body, mesh=mesh, in_specs=in_specs, out_specs=out_specs, check_vma=False)
```

```python
import functools

import jax
import jax.numpy as jnp
from jax import lax
from jax.experimental import pallas as pl
from jax.experimental.pallas import tpu as pltpu
from jax.sharding import PartitionSpec as P

MESH = pl.DeviceIdType.MESH
PARTS = 4
STEPS = (((0, 0, 0, 0),), ((1, 1, 2, 1),), ((2, 3, 1, 3), (3, 2, 3, 2)))
ARRIVE = ((0, 0, 0, 0), (1, 1, 1, 1), (2, 3, 3, 2), (3, 2, 2, 3))


def flip(index, mask):
    out = index
    w = 1
    while w <= mask:
        if mask & w:
            out = out + w - 2 * w * lax.rem(index // w, 2)
        w *= 2
    return out


def kernel(
    n_lat,
    n_seg,
    pos_hbm,
    cnt_hbm,
    coh_hbm,
    semi_ref,
    excess_ref,
    pos_ref,
    cnt_ref,
    coh,
    gath,
    rows_out,
    rows_in,
    col_out,
    col_in,
    sid_in,
    far_rows,
    psum,
    psum_in,
    coh_sem,
    gs_sem,
    gr_sem,
    rs_sem,
    rr_sem,
    cs_sem,
    cr_sem,
    xs_sem,
    xr_sem,
    ss_sem,
    sr_sem,
    ps_sem,
    pr_sem,
    in_sem,
):
    lat = lax.axis_index("lat")
    seg = lax.axis_index("seg")
    slice_bins, width = coh.shape
    points = pos_ref.shape[1]
    blocks = cnt_ref.shape[0]
    block_size = points // blocks
    slots = 2 * points // n_lat
    total_slots = n_lat * slots
    f32, bf16, i32 = jnp.float32, jnp.bfloat16, jnp.int32
    group = n_lat // PARTS
    quarter = lat // group

    def remote(src, dst, send_sem, recv_sem, to):
        return pltpu.make_async_remote_copy(
            src_ref=src,
            dst_ref=dst,
            send_sem=send_sem,
            recv_sem=recv_sem,
            device_id=to,
            device_id_type=MESH,
        )

    barrier = pltpu.get_barrier_semaphore()
    lat_peers = [flip(lat, j) for j in range(n_lat)]
    seg_peers = [flip(seg, m) for m in range(n_seg)]
    far_first = list(range(n_lat - 1, 0, -1))
    seg_far_first = list(range(n_seg - 1, 0, -1))
    for j in far_first:
        pl.semaphore_signal(barrier, inc=1, device_id=(seg, lat_peers[j]), device_id_type=MESH)
    for m in seg_far_first:
        pl.semaphore_signal(barrier, inc=1, device_id=(seg_peers[m], lat), device_id_type=MESH)

    small = [
        pltpu.make_async_copy(pos_hbm, pos_ref, in_sem.at[0]),
        pltpu.make_async_copy(cnt_hbm, cnt_ref, in_sem.at[1]),
    ]
    for copy in small:
        copy.start()
    load = pltpu.make_async_copy(coh_hbm.at[0], coh, coh_sem)
    load.start()
    for copy in small:
        copy.wait()

    pos = pos_ref[...]
    lane = lax.broadcasted_iota(i32, (1, points), 1)
    dest = (pos // 256) // slice_bins
    rel = jnp.bitwise_xor(dest, jnp.full((1, points), lat, i32))
    hits = lax.broadcasted_iota(i32, (n_lat, points), 0) == rel
    hits_f = hits.astype(f32)
    tri = (
        lax.broadcasted_iota(i32, (points, points), 0)
        < lax.broadcasted_iota(i32, (points, points), 1)
    ).astype(f32)
    before = jnp.dot(hits_f.astype(bf16), tri.astype(bf16), preferred_element_type=f32)
    slot = jnp.sum(before * hits_f, axis=0, keepdims=True).astype(i32)
    sid = rel * slots + slot
    limit = jnp.zeros((1, points), i32)
    for b in range(blocks):
        limit = jnp.where(lane // block_size == b, cnt_ref[b], limit)
    valid = (lane % block_size < limit).astype(i32)
    gath[0, 0:1, :] = sid
    gath[0, 1:2, :] = pos
    gath[0, 2:3, :] = valid
    gath[0, 3:4, :] = valid
    pl.semaphore_wait(barrier, n_lat - 1 + n_seg - 1)

    sends = {
        j: remote(gath.at[0], gath.at[j], gs_sem, gr_sem.at[j // group], (seg, lat_peers[j]))
        for j in far_first
    }
    for j in far_first:
        sends[j].start()
    sid_sends = [
        remote(gath.at[0], sid_in.at[m], ss_sem, sr_sem, (seg_peers[m], lat))
        for m in seg_far_first
    ]
    for copy in sid_sends:
        copy.start()

    pos_bits = 8
    bin_bits = (slice_bins - 1).bit_length()
    depth = min(256, slice_bins)
    depth_bits = depth.bit_length() - 1
    base = lat * (slice_bins << pos_bits)
    flag = slice_bins << pos_bits
    sub = lax.broadcasted_iota(i32, (slots, points), 0)
    chunks = slice_bins // depth
    count = jnp.zeros((1, points), i32)
    col = jnp.zeros((1, width), f32)
    late = quarter // 3
    third = quarter // 2 - late
    second = quarter - 2 * third - 3 * late

    def mixed(plain, in_second, in_third, in_last):
        return (
            plain
            + second * (in_second - plain)
            + third * (in_third - plain)
            + late * (in_last - plain)
        )

    def order(turns):
        first = mixed(*turns) * group
        peers = [mixed(*(lat_peers[g * group + i] for g in turns)) for i in range(group)]
        return first, peers

    def hand_on(src, j, g):
        for m in seg_far_first:
            copy = remote(
                src, far_rows.at[m, j], xs_sem, xr_sem.at[g], (seg_peers[m], lat)
            )
            copy.start()

    parity = lax.rem(lat, 2)
    for step, turns in enumerate(STEPS):
        places = [order(t) if step else (0, lat_peers[:group]) for t in turns]
        cols = []
        for first, peers in places:
            rng = pl.ds(first, group) if step else pl.ds(1, group - 1)
            remote(
                gath.at[rng], gath.at[rng], gs_sem, gr_sem.at[first // group], (seg, peers[-1])
            ).wait_recv()
            for i in range(group):
                j = first + i
                live_row = gath[j, 2:3, :]
                code = (gath[j, 1:2, :] - base + flag * (1 + live_row)).astype(f32)
                here = (gath[j, 0:1, :] - j * slots) == sub
                cols.append(jnp.sum(jnp.where(here, code, 0.0), axis=1, keepdims=True))
                count = count + live_row
        code = jnp.concatenate(cols, axis=0).astype(i32)
        kind = lax.shift_right_logical(code, bin_bits + pos_bits)
        low = lax.shift_right_logical(code & (flag - 1), pos_bits)
        upper = (code & ((1 << pos_bits) - 1)).astype(f32) * (1.0 / (1 << pos_bits))
        chunk = jnp.where(kind > 0, lax.shift_right_logical(low, depth_bits), -2)
        in_chunk = low & (depth - 1)
        bins = lax.broadcasted_iota(i32, (code.shape[0], depth), 1)
        zero = jnp.zeros(bins.shape, bf16)
        local = jnp.where(bins == in_chunk, 1.0 - upper, 0.0)
        local = jnp.where(bins == ((in_chunk + 1) & (depth - 1)), upper, local).astype(bf16)
        where_id = jnp.where(bins < in_chunk, chunk + 1, chunk).astype(f32).astype(bf16)
        if step == 0:
            load.wait()
        weights = jnp.concatenate(
            [jnp.where(where_id == jnp.asarray(c, bf16), local, zero) for c in range(chunks)],
            axis=1,
        )
        held = jnp.dot(weights, coh[...], preferred_element_type=f32)
        for n, (first, peers) in enumerate(places):
            for i in range(group):
                at = (n * group + i) * slots
                rows_out[first + i] = held[at : at + slots, :]
            if step == 0:
                for j in range(1, group):
                    remote(
                        rows_out.at[j], rows_in.at[j], rs_sem, rr_sem.at[j], (seg, lat_peers[j])
                    ).start()
                hand_on(rows_out.at[0], 0, 0)
                continue
            for i in range(group):
                turn = parity if i % 2 == 0 else -parity
                j = first + i + turn
                peer = peers[i] + parity * (peers[i ^ 1] - peers[i])
                remote(
                    rows_out.at[j], rows_in.at[j], rs_sem, rr_sem.at[j], (seg, peer)
                ).start()
        col = col + jnp.sum(jnp.where(kind > 1, held, 0.0), axis=0, keepdims=True)
    col_out[0] = col
    for m in seg_far_first:
        remote(col_out.at[0], psum_in.at[m], ps_sem, pr_sem, (seg_peers[m], lat)).start()
    total_count = jnp.sum(count.astype(f32), axis=1, keepdims=True)

    for g, turns in enumerate(ARRIVE):
        first, peers = order(turns) if g else (0, lat_peers[:group])
        for i in range(group):
            j = first + i
            if g or i:
                remote(
                    rows_out.at[j], rows_in.at[j], rs_sem, rr_sem.at[j], (seg, peers[i])
                ).wait_recv()
                hand_on(rows_in.at[j], j, first // group)

    def tree(terms):
        w = 1
        while w < n_seg:
            terms = [terms[i] + terms[i + 1] for i in range(0, len(terms), 2)]
            w *= 2
        return terms[0]

    rng = pl.ds(1, n_lat - 1)
    seg_rng = pl.ds(1, n_seg - 1)
    psums = remote(psum_in.at[seg_rng], psum_in.at[seg_rng], ps_sem, pr_sem, (seg_peers[1], lat))
    psums.wait_recv()
    col = tree([col] + [psum_in[m] for m in range(1, n_seg)])
    psum[0] = col
    for j in far_first:
        remote(psum.at[0], col_in.at[j], cs_sem, cr_sem, (seg, lat_peers[j])).start()
    cols = remote(col_in.at[rng], col_in.at[rng], cs_sem, cr_sem, (seg, lat_peers[1]))

    sids = remote(sid_in.at[seg_rng], sid_in.at[seg_rng], ss_sem, sr_sem, (seg_peers[1], lat))
    sids.wait_recv()
    slot_row = lax.broadcasted_iota(i32, (total_slots, points), 0)
    picks = []
    for m in range(n_seg):
        theirs = sid_in[m, 0:1, :] if m else sid
        picks.append((slot_row == theirs).astype(f32).T.astype(bf16))
    remote(gath.at[rng], gath.at[rng], gs_sem, gr_sem.at[0], (seg, lat_peers[1])).wait_send()
    remote(rows_out.at[rng], rows_in.at[rng], rs_sem, rr_sem.at[0], (seg, lat_peers[1])).wait_send()
    psums.wait_send()
    sids.wait_send()

    total = jnp.zeros((points, width), f32)
    for part_id in range(PARTS):
        first = part_id * group
        theirs = far_rows.at[seg_rng, pl.ds(first, group)]
        remote(theirs, theirs, xs_sem, xr_sem.at[part_id], (seg_peers[1], lat)).wait_recv()
        got = []
        mine = []
        for m in range(n_seg):
            mine.append(picks[m][:, first * slots : (first + group) * slots])
            for j in range(first, first + group):
                if m:
                    got.append(far_rows[m, j])
                else:
                    got.append(rows_in[j] if j else rows_out[0])
        got = jnp.concatenate(got, axis=0)
        high = got.astype(bf16)
        rest = (got - high.astype(f32)).astype(bf16)
        total = total + jnp.dot(
            jnp.concatenate(mine + mine, axis=1),
            jnp.concatenate([high, rest], axis=0),
            preferred_element_type=f32,
        )
    stat = total / n_seg
    semi_ref[...] = stat.astype(semi_ref.dtype)
    cols.wait_recv()
    for j in range(1, n_lat):
        col = col + col_in[j]
    global_mean = (col / n_seg) / total_count
    row = lax.broadcasted_iota(i32, (block_size, width), 0)
    for b in range(blocks):
        block = stat[b * block_size : (b + 1) * block_size]
        block_sum = jnp.sum(jnp.where(row < cnt_ref[b], block, 0.0), axis=0, keepdims=True)
        mean = block_sum / jnp.full((1, width), cnt_ref[b], i32).astype(f32)
        excess_ref[b : b + 1, :] = mean - global_mean

    cols.wait_send()
    theirs = far_rows.at[seg_rng]
    remote(theirs, theirs, xs_sem, xr_sem.at[0], (seg_peers[1], lat)).wait_send()


def deliver(semi_ref, excess_ref, semi_out, excess_out, sem):
    copies = [
        pltpu.make_async_copy(semi_ref, semi_out, sem.at[0]),
        pltpu.make_async_copy(excess_ref, excess_out, sem.at[1]),
    ]
    for copy in copies:
        copy.start()
    for copy in copies:
        copy.wait()


def shards(n_lat, n_seg, coh_map, positions, counts):
    _, slice_bins, width = coh_map.shape
    points = positions.shape[1]
    blocks = counts.shape[0]
    slots = 2 * points // n_lat
    f32 = jnp.float32
    dma = pltpu.SemaphoreType.DMA
    made = pl.pallas_call(
        functools.partial(kernel, n_lat, n_seg),
        out_shape=(
            pltpu.VMEM((points, width), jnp.bfloat16),
            pltpu.VMEM((blocks, width), f32),
        ),
        in_specs=[
            pl.BlockSpec(memory_space=pl.ANY),
            pl.BlockSpec(memory_space=pl.ANY),
            pl.BlockSpec(memory_space=pl.ANY),
        ],
        out_specs=(
            pl.BlockSpec(memory_space=pltpu.VMEM),
            pl.BlockSpec(memory_space=pltpu.VMEM),
        ),
        scratch_shapes=[
            pltpu.VMEM((1, points), jnp.int32),
            pltpu.SMEM((blocks,), jnp.int32),
            pltpu.VMEM((slice_bins, width), coh_map.dtype),
            pltpu.VMEM((n_lat, 4, points), jnp.int32),
            pltpu.VMEM((n_lat, slots, width), f32),
            pltpu.VMEM((n_lat, slots, width), f32),
            pltpu.VMEM((1, 1, width), f32),
            pltpu.VMEM((n_lat, 1, width), f32),
            pltpu.VMEM((n_seg, 4, points), jnp.int32),
            pltpu.VMEM((n_seg, n_lat, slots, width), f32),
            pltpu.VMEM((1, 1, width), f32),
            pltpu.VMEM((n_seg, 1, width), f32),
            dma,
            dma,
            dma((PARTS,)),
            dma,
            dma((n_lat,)),
            dma,
            dma,
            dma,
            dma((PARTS,)),
            dma,
            dma,
            dma,
            dma,
            dma((2,)),
        ],
        compiler_params=pltpu.CompilerParams(collective_id=0, has_side_effects=True),
    )(positions, counts, coh_map)
    made = [pltpu.with_memory_space_constraint(x, pltpu.VMEM) for x in made]
    return pl.pallas_call(
        deliver,
        out_shape=tuple(jax.ShapeDtypeStruct(x.shape, x.dtype) for x in made),
        in_specs=[pl.BlockSpec(memory_space=pltpu.VMEM)] * 2,
        out_specs=(pl.BlockSpec(memory_space=pl.ANY),) * 2,
        scratch_shapes=[dma((2,))],
    )(*made)


def solution(mesh):
    in_specs = (P("seg", "lat", None), P("seg", "lat"), P("lat"))
    out_specs = (P("lat", None), P("lat", None))
    body = functools.partial(shards, mesh.shape["lat"], mesh.shape["seg"])
    return jax.shard_map(body, mesh=mesh, in_specs=in_specs, out_specs=out_specs, check_vma=False)
```

```python
import functools

import jax
import jax.numpy as jnp
from jax import lax
from jax.experimental import pallas as pl
from jax.experimental.pallas import tpu as pltpu
from jax.sharding import PartitionSpec as P

MESH = pl.DeviceIdType.MESH
PARTS = 4
DIRECT = ((0, 1), (0, 3), (1, 2))
STEPS = (((0, 0, 0, 0),), ((1, 1, 2, 1),), ((2, 3, 1, 3), (3, 2, 3, 2)))
ARRIVE = ((0, 0, 0, 0), (1, 1, 1, 1), (2, 3, 3, 2), (3, 2, 2, 3))


def flip(index, mask):
    out = index
    w = 1
    while w <= mask:
        if mask & w:
            out = out + w - 2 * w * lax.rem(index // w, 2)
        w *= 2
    return out


def kernel(
    n_lat,
    n_seg,
    pos_hbm,
    cnt_hbm,
    coh_hbm,
    semi_ref,
    excess_ref,
    pos_ref,
    cnt_ref,
    coh,
    gath,
    rows_out,
    rows_in,
    col_out,
    col_in,
    sid_in,
    far_rows,
    psum,
    psum_in,
    coh_sem,
    gs_sem,
    gr_sem,
    rs_sem,
    rr_sem,
    cs_sem,
    cr_sem,
    xs_sem,
    xr_sem,
    ss_sem,
    sr_sem,
    ps_sem,
    pr_sem,
    in_sem,
    ds_sem,
):
    lat = lax.axis_index("lat")
    seg = lax.axis_index("seg")
    slice_bins, width = coh.shape
    points = pos_ref.shape[1]
    blocks = cnt_ref.shape[0]
    block_size = points // blocks
    slots = 2 * points // n_lat
    total_slots = n_lat * slots
    f32, bf16, i32 = jnp.float32, jnp.bfloat16, jnp.int32
    group = n_lat // PARTS
    quarter = lat // group
    parity = lax.rem(lat, 2)
    late = quarter // 3
    third = quarter // 2 - late
    second = quarter - 2 * third - 3 * late
    is_quarter = (1 - second - third - late, second, third, late)

    def remote(src, dst, send_sem, recv_sem, to):
        return pltpu.make_async_remote_copy(
            src_ref=src,
            dst_ref=dst,
            send_sem=send_sem,
            recv_sem=recv_sem,
            device_id=to,
            device_id_type=MESH,
        )

    barrier = pltpu.get_barrier_semaphore()
    lat_peers = [flip(lat, j) for j in range(n_lat)]
    seg_peers = [flip(seg, m) for m in range(n_seg)]
    far_first = list(range(n_lat - 1, 0, -1))
    seg_far_first = list(range(n_seg - 1, 0, -1))
    for j in far_first:
        pl.semaphore_signal(barrier, inc=1, device_id=(seg, lat_peers[j]), device_id_type=MESH)
    for m in seg_far_first:
        pl.semaphore_signal(barrier, inc=1, device_id=(seg_peers[m], lat), device_id_type=MESH)

    for owner, g in DIRECT:

        @pl.when((quarter == owner) & (parity == 0))
        def _(g=g):
            for j in range(g * group, (g + 1) * group):
                pl.semaphore_signal(
                    barrier, inc=1, device_id=(seg_peers[-1], lat_peers[j]), device_id_type=MESH
                )

    small = [
        pltpu.make_async_copy(pos_hbm, pos_ref, in_sem.at[0]),
        pltpu.make_async_copy(cnt_hbm, cnt_ref, in_sem.at[1]),
    ]
    for copy in small:
        copy.start()
    load = pltpu.make_async_copy(coh_hbm.at[0], coh, coh_sem)
    load.start()
    for copy in small:
        copy.wait()

    pos = pos_ref[...]
    lane = lax.broadcasted_iota(i32, (1, points), 1)
    dest = (pos // 256) // slice_bins
    rel = jnp.bitwise_xor(dest, jnp.full((1, points), lat, i32))
    hits = lax.broadcasted_iota(i32, (n_lat, points), 0) == rel
    hits_f = hits.astype(f32)
    tri = (
        lax.broadcasted_iota(i32, (points, points), 0)
        < lax.broadcasted_iota(i32, (points, points), 1)
    ).astype(f32)
    before = jnp.dot(hits_f.astype(bf16), tri.astype(bf16), preferred_element_type=f32)
    slot = jnp.sum(before * hits_f, axis=0, keepdims=True).astype(i32)
    sid = rel * slots + slot
    limit = jnp.zeros((1, points), i32)
    for b in range(blocks):
        limit = jnp.where(lane // block_size == b, cnt_ref[b], limit)
    valid = (lane % block_size < limit).astype(i32)
    gath[0, 0:1, :] = sid
    gath[0, 1:2, :] = pos
    gath[0, 2:3, :] = valid
    gath[0, 3:4, :] = valid

    straight = sum(is_quarter[owner ^ g] for owner, g in DIRECT)
    pl.semaphore_wait(barrier, n_lat - 1 + n_seg - 1 + straight * (group // 2))

    sends = {
        j: remote(gath.at[0], gath.at[j], gs_sem, gr_sem.at[j // group], (seg, lat_peers[j]))
        for j in far_first
    }
    for j in far_first:
        sends[j].start()
    sid_sends = [
        remote(gath.at[0], sid_in.at[m], ss_sem, sr_sem, (seg_peers[m], lat))
        for m in seg_far_first
    ]
    for copy in sid_sends:
        copy.start()

    pos_bits = 8
    bin_bits = (slice_bins - 1).bit_length()
    depth = min(256, slice_bins)
    depth_bits = depth.bit_length() - 1
    base = lat * (slice_bins << pos_bits)
    flag = slice_bins << pos_bits
    sub = lax.broadcasted_iota(i32, (slots, points), 0)
    chunks = slice_bins // depth
    count = jnp.zeros((1, points), i32)
    col = jnp.zeros((1, width), f32)
    def mixed(plain, in_second, in_third, in_last):
        return (
            plain
            + second * (in_second - plain)
            + third * (in_third - plain)
            + late * (in_last - plain)
        )

    def order(turns):
        first = mixed(*turns) * group
        peers = [mixed(*(lat_peers[g * group + i] for g in turns)) for i in range(group)]
        return first, peers

    def hand_on(src, j, g, turn=0):
        for m in seg_far_first:
            copy = remote(
                src, far_rows.at[m * n_lat + j], xs_sem, xr_sem.at[g], (seg_peers[m], lat)
            )
            skips = [owner for owner, r in DIRECT if ARRIVE[turn][owner] == r]
            if turn and skips and m == n_seg - 1:
                skip = sum(is_quarter[owner] for owner in skips) * (1 - parity)
                pl.when(skip == 0)(copy.start)
            else:
                copy.start()

    for step, turns in enumerate(STEPS):
        places = [order(t) if step else (0, lat_peers[:group]) for t in turns]
        cols = []
        for first, peers in places:
            rng = pl.ds(first, group) if step else pl.ds(1, group - 1)
            remote(
                gath.at[rng], gath.at[rng], gs_sem, gr_sem.at[first // group], (seg, peers[-1])
            ).wait_recv()
            for i in range(group):
                j = first + i
                live_row = gath[j, 2:3, :]
                code = (gath[j, 1:2, :] - base + flag * (1 + live_row)).astype(f32)
                here = (gath[j, 0:1, :] - j * slots) == sub
                cols.append(jnp.sum(jnp.where(here, code, 0.0), axis=1, keepdims=True))
                count = count + live_row
        code = jnp.concatenate(cols, axis=0).astype(i32)
        kind = lax.shift_right_logical(code, bin_bits + pos_bits)
        low = lax.shift_right_logical(code & (flag - 1), pos_bits)
        upper = (code & ((1 << pos_bits) - 1)).astype(f32) * (1.0 / (1 << pos_bits))
        chunk = jnp.where(kind > 0, lax.shift_right_logical(low, depth_bits), -2)
        in_chunk = low & (depth - 1)
        bins = lax.broadcasted_iota(i32, (code.shape[0], depth), 1)
        zero = jnp.zeros(bins.shape, bf16)
        local = jnp.where(bins == in_chunk, 1.0 - upper, 0.0)
        local = jnp.where(bins == ((in_chunk + 1) & (depth - 1)), upper, local).astype(bf16)
        where_id = jnp.where(bins < in_chunk, chunk + 1, chunk).astype(f32).astype(bf16)
        if step == 0:
            load.wait()
        weights = jnp.concatenate(
            [jnp.where(where_id == jnp.asarray(c, bf16), local, zero) for c in range(chunks)],
            axis=1,
        )
        held = jnp.dot(weights, coh[...], preferred_element_type=f32)
        posts, crosses = [], []
        for n, (first, peers) in enumerate(places):
            for i in range(group):
                at = (n * group + i) * slots
                rows_out[first + i] = held[at : at + slots, :]
            if step == 0:
                for j in range(1, group):
                    remote(
                        rows_out.at[j], rows_in.at[j], rs_sem, rr_sem.at[j], (seg, lat_peers[j])
                    ).start()
                hand_on(rows_out.at[0], 0, 0)
                continue
            def post(odd, first=first, peers=peers):
                for i in range(odd, group, 2):
                    turn = parity if odd == 0 else -parity
                    j = first + i + turn
                    peer = peers[i] + parity * (peers[i ^ 1] - peers[i])
                    remote(
                        rows_out.at[j], rows_in.at[j], rs_sem, rr_sem.at[j], (seg, peer)
                    ).start()

            def across(first=first, peers=peers):
                for i in range(0, group, 2):
                    j = first + i + parity
                    peer = peers[i] + parity * (peers[i + 1] - peers[i])
                    remote(
                        rows_out.at[j],
                        far_rows.at[(n_seg - 1) * n_lat + j],
                        ds_sem,
                        xr_sem.at[first // group],
                        (seg_peers[-1], peer),
                    ).start()

            posts.append(post)
            crosses.append(across)
        for what, n in ((0, 0), (1, 0), (2, 0), (0, 1), (1, 1), (2, 1)) if step == 2 else ((0, 0), (1, 0), (2, 0)) if step else ():
            if what < 2:
                posts[n](what)
                continue
            makers = [owner ^ r for owner, r in DIRECT if turns[n][owner ^ r] == r]
            if makers:
                pl.when(sum(is_quarter[q] for q in makers) == 1)(crosses[n])
        col = col + jnp.sum(jnp.where(kind > 1, held, 0.0), axis=0, keepdims=True)
    col_out[0] = col
    for m in seg_far_first:
        remote(col_out.at[0], psum_in.at[m], ps_sem, pr_sem, (seg_peers[m], lat)).start()
    total_count = jnp.sum(count.astype(f32), axis=1, keepdims=True)

    def tree(terms):
        w = 1
        while w < n_seg:
            terms = [terms[i] + terms[i + 1] for i in range(0, len(terms), 2)]
            w *= 2
        return terms[0]

    rng = pl.ds(1, n_lat - 1)
    seg_rng = pl.ds(1, n_seg - 1)
    psums = remote(psum_in.at[seg_rng], psum_in.at[seg_rng], ps_sem, pr_sem, (seg_peers[1], lat))
    cols = remote(col_in.at[rng], col_in.at[rng], cs_sem, cr_sem, (seg, lat_peers[1]))
    for turn, turns in enumerate(ARRIVE):
        if turn == 2:
            psums.wait_recv()
            col = tree([col] + [psum_in[m] for m in range(1, n_seg)])
            psum[0] = col
            for j in far_first:
                remote(psum.at[0], col_in.at[j], cs_sem, cr_sem, (seg, lat_peers[j])).start()
        first, peers = order(turns) if turn else (0, lat_peers[:group])
        for i in range(group):
            j = first + i
            if turn or i:
                remote(
                    rows_out.at[j], rows_in.at[j], rs_sem, rr_sem.at[j], (seg, peers[i])
                ).wait_recv()
                hand_on(rows_in.at[j], j, first // group, turn)

    sids = remote(sid_in.at[seg_rng], sid_in.at[seg_rng], ss_sem, sr_sem, (seg_peers[1], lat))
    sids.wait_recv()
    slot_row = lax.broadcasted_iota(i32, (total_slots, points), 0)
    picks = []
    for m in range(n_seg):
        theirs = sid_in[m, 0:1, :] if m else sid
        picks.append((slot_row == theirs).astype(f32).T.astype(bf16))
    remote(gath.at[rng], gath.at[rng], gs_sem, gr_sem.at[0], (seg, lat_peers[1])).wait_send()
    remote(rows_out.at[rng], rows_in.at[rng], rs_sem, rr_sem.at[0], (seg, lat_peers[1])).wait_send()
    psums.wait_send()
    sids.wait_send()

    total = jnp.zeros((points, width), f32)
    for part_id in range(PARTS):
        first = part_id * group
        theirs = far_rows.at[pl.ds(0, (n_seg - 1) * group)]
        remote(theirs, theirs, xs_sem, xr_sem.at[part_id], (seg_peers[1], lat)).wait_recv()
        got = []
        mine = []
        for m in range(n_seg):
            mine.append(picks[m][:, first * slots : (first + group) * slots])
            for j in range(first, first + group):
                if m:
                    got.append(far_rows[m * n_lat + j])
                else:
                    got.append(rows_in[j] if j else rows_out[0])
        got = jnp.concatenate(got, axis=0)
        high = got.astype(bf16)
        rest = (got - high.astype(f32)).astype(bf16)
        total = total + jnp.dot(
            jnp.concatenate(mine + mine, axis=1),
            jnp.concatenate([high, rest], axis=0),
            preferred_element_type=f32,
        )
    stat = total / n_seg
    semi_ref[...] = stat.astype(semi_ref.dtype)
    cols.wait_recv()
    for j in range(1, n_lat):
        col = col + col_in[j]
    global_mean = (col / n_seg) / total_count
    row = lax.broadcasted_iota(i32, (block_size, width), 0)
    for b in range(blocks):
        block = stat[b * block_size : (b + 1) * block_size]
        block_sum = jnp.sum(jnp.where(row < cnt_ref[b], block, 0.0), axis=0, keepdims=True)
        mean = block_sum / jnp.full((1, width), cnt_ref[b], i32).astype(f32)
        excess_ref[b : b + 1, :] = mean - global_mean

    cols.wait_send()

    def sent(blocks, sem):
        ref = far_rows.at[pl.ds(0, blocks)]
        remote(ref, ref, sem, xr_sem.at[0], (seg_peers[1], lat)).wait_send()

    for q in range(PARTS):
        skipped = group * sum(owner == q for owner, _ in DIRECT)
        across = group // 2 * sum(owner ^ g == q for owner, g in DIRECT)
        for core in range(2):

            @pl.when((quarter == q) & (parity == core))
            def _(skipped=skipped, across=across, core=core):
                sent((n_seg - 1) * n_lat - (0 if core else skipped), xs_sem)
                if across:
                    sent(across, ds_sem)


def deliver(semi_ref, excess_ref, semi_out, excess_out, sem):
    copies = [
        pltpu.make_async_copy(semi_ref, semi_out, sem.at[0]),
        pltpu.make_async_copy(excess_ref, excess_out, sem.at[1]),
    ]
    for copy in copies:
        copy.start()
    for copy in copies:
        copy.wait()


def shards(n_lat, n_seg, coh_map, positions, counts):
    _, slice_bins, width = coh_map.shape
    points = positions.shape[1]
    blocks = counts.shape[0]
    slots = 2 * points // n_lat
    f32 = jnp.float32
    dma = pltpu.SemaphoreType.DMA
    made = pl.pallas_call(
        functools.partial(kernel, n_lat, n_seg),
        out_shape=(
            pltpu.VMEM((points, width), jnp.bfloat16),
            pltpu.VMEM((blocks, width), f32),
        ),
        in_specs=[
            pl.BlockSpec(memory_space=pl.ANY),
            pl.BlockSpec(memory_space=pl.ANY),
            pl.BlockSpec(memory_space=pl.ANY),
        ],
        out_specs=(
            pl.BlockSpec(memory_space=pltpu.VMEM),
            pl.BlockSpec(memory_space=pltpu.VMEM),
        ),
        scratch_shapes=[
            pltpu.VMEM((1, points), jnp.int32),
            pltpu.SMEM((blocks,), jnp.int32),
            pltpu.VMEM((slice_bins, width), coh_map.dtype),
            pltpu.VMEM((n_lat, 4, points), jnp.int32),
            pltpu.VMEM((n_lat, slots, width), f32),
            pltpu.VMEM((n_lat, slots, width), f32),
            pltpu.VMEM((1, 1, width), f32),
            pltpu.VMEM((n_lat, 1, width), f32),
            pltpu.VMEM((n_seg, 4, points), jnp.int32),
            pltpu.VMEM((n_seg * n_lat, slots, width), f32),
            pltpu.VMEM((1, 1, width), f32),
            pltpu.VMEM((n_seg, 1, width), f32),
            dma,
            dma,
            dma((PARTS,)),
            dma,
            dma((n_lat,)),
            dma,
            dma,
            dma,
            dma((PARTS,)),
            dma,
            dma,
            dma,
            dma,
            dma((2,)),
            dma,
        ],
        compiler_params=pltpu.CompilerParams(collective_id=0, has_side_effects=True),
    )(positions, counts, coh_map)
    made = [pltpu.with_memory_space_constraint(x, pltpu.VMEM) for x in made]
    return pl.pallas_call(
        deliver,
        out_shape=tuple(jax.ShapeDtypeStruct(x.shape, x.dtype) for x in made),
        in_specs=[pl.BlockSpec(memory_space=pltpu.VMEM)] * 2,
        out_specs=(pl.BlockSpec(memory_space=pl.ANY),) * 2,
        scratch_shapes=[dma((2,))],
    )(*made)


def solution(mesh):
    in_specs = (P("seg", "lat", None), P("seg", "lat"), P("lat"))
    out_specs = (P("lat", None), P("lat", None))
    body = functools.partial(shards, mesh.shape["lat"], mesh.shape["seg"])
    return jax.shard_map(body, mesh=mesh, in_specs=in_specs, out_specs=out_specs, check_vma=False)
```

```python
import functools

import jax
import jax.numpy as jnp
from jax import lax
from jax.experimental import pallas as pl
from jax.experimental.pallas import tpu as pltpu
from jax.sharding import PartitionSpec as P

MESH = pl.DeviceIdType.MESH
PARTS = 4
DIRECT = ((0, 1), (0, 3), (1, 2))
STEPS = (((0, 0, 0, 0),), ((1, 1, 2, 1),), ((2, 3, 1, 3), (3, 2, 3, 2)))
ARRIVE = ((0, 0, 0, 0), (1, 1, 1, 1), (2, 3, 3, 2), (3, 2, 2, 3))


def flip(index, mask):
    out = index
    w = 1
    while w <= mask:
        if mask & w:
            out = out + w - 2 * w * lax.rem(index // w, 2)
        w *= 2
    return out


def kernel(
    n_lat,
    n_seg,
    pos_hbm,
    cnt_hbm,
    coh_hbm,
    semi_ref,
    excess_ref,
    pos_ref,
    cnt_ref,
    coh,
    gath,
    rows_out,
    rows_in,
    col_out,
    col_in,
    far_rows,
    psum,
    coh_sem,
    gs_sem,
    gr_sem,
    rs_sem,
    rr_sem,
    cs_sem,
    cr_sem,
    xr_sem,
    sr_sem,
    pr_sem,
    in_sem,
):
    lat = lax.axis_index("lat")
    seg = lax.axis_index("seg")
    slice_bins, width = coh.shape
    points = pos_ref.shape[1]
    blocks = cnt_ref.shape[0]
    block_size = points // blocks
    slots = 2 * points // n_lat
    total_slots = n_lat * slots
    f32, bf16, i32 = jnp.float32, jnp.bfloat16, jnp.int32
    group = n_lat // PARTS
    quarter = lat // group
    parity = lax.rem(lat, 2)
    late = quarter // 3
    third = quarter // 2 - late
    second = quarter - 2 * third - 3 * late
    is_quarter = (1 - second - third - late, second, third, late)

    def remote(src, dst, send_sem, recv_sem, to):
        return pltpu.make_async_remote_copy(
            src_ref=src,
            dst_ref=dst,
            send_sem=send_sem,
            recv_sem=recv_sem,
            device_id=to,
            device_id_type=MESH,
        )

    barrier = pltpu.get_barrier_semaphore()
    lat_peers = [flip(lat, j) for j in range(n_lat)]
    seg_peers = [flip(seg, m) for m in range(n_seg)]
    far_first = list(range(n_lat - 1, 0, -1))
    seg_far_first = list(range(n_seg - 1, 0, -1))
    for j in far_first:
        pl.semaphore_signal(barrier, inc=1, device_id=(seg, lat_peers[j]), device_id_type=MESH)
    for m in seg_far_first:
        pl.semaphore_signal(barrier, inc=1, device_id=(seg_peers[m], lat), device_id_type=MESH)

    for owner, g in DIRECT:

        @pl.when((quarter == owner) & (parity == 0))
        def _(g=g):
            for j in range(g * group, (g + 1) * group):
                pl.semaphore_signal(
                    barrier, inc=1, device_id=(seg_peers[-1], lat_peers[j]), device_id_type=MESH
                )

    small = [
        pltpu.make_async_copy(pos_hbm, pos_ref, in_sem.at[0]),
        pltpu.make_async_copy(cnt_hbm, cnt_ref, in_sem.at[1]),
    ]
    for copy in small:
        copy.start()
    load = pltpu.make_async_copy(coh_hbm.at[0], coh, coh_sem)
    load.start()
    for copy in small:
        copy.wait()

    pos = pos_ref[...]
    lane = lax.broadcasted_iota(i32, (1, points), 1)
    dest = (pos // 256) // slice_bins
    rel = jnp.bitwise_xor(dest, jnp.full((1, points), lat, i32))
    hits = lax.broadcasted_iota(i32, (n_lat, points), 0) == rel
    hits_f = hits.astype(f32)
    tri = (
        lax.broadcasted_iota(i32, (points, points), 0)
        < lax.broadcasted_iota(i32, (points, points), 1)
    ).astype(f32)
    before = jnp.dot(hits_f.astype(bf16), tri.astype(bf16), preferred_element_type=f32)
    slot = jnp.sum(before * hits_f, axis=0, keepdims=True).astype(i32)
    sid = rel * slots + slot
    limit = jnp.zeros((1, points), i32)
    for b in range(blocks):
        limit = jnp.where(lane // block_size == b, cnt_ref[b], limit)
    valid = (lane % block_size < limit).astype(i32)
    gath[0, 0:1, :] = sid
    gath[0, 1:2, :] = pos
    gath[0, 2:3, :] = valid
    gath[0, 3:4, :] = valid

    straight = sum(is_quarter[owner ^ g] for owner, g in DIRECT)
    pl.semaphore_wait(barrier, n_lat - 1 + n_seg - 1 + straight * (group // 2))

    sends = {
        j: remote(gath.at[0], gath.at[j], gs_sem, gr_sem.at[j // group], (seg, lat_peers[j]))
        for j in far_first
    }
    for j in far_first:
        sends[j].start()
    sid_sends = [
        remote(gath.at[0], gath.at[n_lat + m], gs_sem, sr_sem, (seg_peers[m], lat))
        for m in seg_far_first
    ]
    for copy in sid_sends:
        copy.start()

    pos_bits = 8
    bin_bits = (slice_bins - 1).bit_length()
    depth = min(256, slice_bins)
    depth_bits = depth.bit_length() - 1
    base = lat * (slice_bins << pos_bits)
    flag = slice_bins << pos_bits
    sub = lax.broadcasted_iota(i32, (slots, points), 0)
    chunks = slice_bins // depth
    count = jnp.zeros((1, points), i32)
    col = jnp.zeros((1, width), f32)

    def mixed(plain, in_second, in_third, in_last):
        return (
            plain
            + second * (in_second - plain)
            + third * (in_third - plain)
            + late * (in_last - plain)
        )

    def order(turns):
        first = mixed(*turns) * group
        peers = [mixed(*(lat_peers[g * group + i] for g in turns)) for i in range(group)]
        return first, peers

    def hand_on(src, j, g, turn=0):
        for m in seg_far_first:
            copy = remote(
                src, far_rows.at[m * n_lat + j], rs_sem, xr_sem.at[g - (g + PARTS - 1) // PARTS], (seg_peers[m], lat)
            )
            skips = [owner for owner, r in DIRECT if ARRIVE[turn][owner] == r]
            if turn and skips and m == n_seg - 1:
                skip = sum(is_quarter[owner] for owner in skips) * (1 - parity)
                pl.when(skip == 0)(copy.start)
            else:
                copy.start()

    for step, turns in enumerate(STEPS):
        places = [order(t) if step else (0, lat_peers[:group]) for t in turns]
        cols = []
        for first, peers in places:
            rng = pl.ds(first, group) if step else pl.ds(1, group - 1)
            remote(
                gath.at[rng], gath.at[rng], gs_sem, gr_sem.at[first // group], (seg, peers[-1])
            ).wait_recv()
            for i in range(group):
                j = first + i
                live_row = gath[j, 2:3, :]
                code = (gath[j, 1:2, :] - base + flag * (1 + live_row)).astype(f32)
                here = (gath[j, 0:1, :] - j * slots) == sub
                cols.append(jnp.sum(jnp.where(here, code, 0.0), axis=1, keepdims=True))
                count = count + live_row
        code = jnp.concatenate(cols, axis=0).astype(i32)
        kind = lax.shift_right_logical(code, bin_bits + pos_bits)
        low = lax.shift_right_logical(code & (flag - 1), pos_bits)
        upper = (code & ((1 << pos_bits) - 1)).astype(f32) * (1.0 / (1 << pos_bits))
        chunk = jnp.where(kind > 0, lax.shift_right_logical(low, depth_bits), -2)
        in_chunk = low & (depth - 1)
        bins = lax.broadcasted_iota(i32, (code.shape[0], depth), 1)
        zero = jnp.zeros(bins.shape, bf16)
        local = jnp.where(bins == in_chunk, 1.0 - upper, 0.0)
        local = jnp.where(bins == ((in_chunk + 1) & (depth - 1)), upper, local).astype(bf16)
        where_id = jnp.where(bins < in_chunk, chunk + 1, chunk).astype(f32).astype(bf16)
        if step == 0:
            load.wait()
        weights = jnp.concatenate(
            [jnp.where(where_id == jnp.asarray(c, bf16), local, zero) for c in range(chunks)],
            axis=1,
        )
        held = jnp.dot(weights, coh[...], preferred_element_type=f32)
        posts, crosses = [], []
        for n, (first, peers) in enumerate(places):
            for i in range(group):
                at = (n * group + i) * slots
                rows_out[first + i] = held[at : at + slots, :]
            if step == 0:
                for j in range(1, group):
                    remote(
                        rows_out.at[j], rows_in.at[j], rs_sem, rr_sem.at[j - 1], (seg, lat_peers[j])
                    ).start()
                hand_on(rows_out.at[0], 0, 0)
                continue
            def post(odd, first=first, peers=peers):
                for i in range(odd, group, 2):
                    turn = parity if odd == 0 else -parity
                    j = first + i + turn
                    peer = peers[i] + parity * (peers[i ^ 1] - peers[i])
                    remote(
                        rows_out.at[j], rows_in.at[j], rs_sem, rr_sem.at[j - 1], (seg, peer)
                    ).start()

            def across(first=first, peers=peers):
                for i in range(0, group, 2):
                    j = first + i + parity
                    peer = peers[i] + parity * (peers[i + 1] - peers[i])
                    remote(
                        rows_out.at[j],
                        far_rows.at[(n_seg - 1) * n_lat + j],
                        rs_sem,
                        xr_sem.at[first // group - 1],
                        (seg_peers[-1], peer),
                    ).start()

            posts.append(post)
            crosses.append(across)
        for what, n in ((0, 0), (1, 0), (1, 1), (2, 0), (0, 1), (2, 1)) if step == 2 else ((0, 0), (1, 0), (2, 0)) if step else ():
            if what < 2:
                posts[n](what)
                continue
            makers = [owner ^ r for owner, r in DIRECT if turns[n][owner ^ r] == r]
            if makers:
                pl.when(sum(is_quarter[q] for q in makers) == 1)(crosses[n])
        col = col + jnp.sum(jnp.where(kind > 1, held, 0.0), axis=0, keepdims=True)
    col_out[0] = col
    for m in seg_far_first:
        remote(col_out.at[0], col_in.at[n_lat + m], cs_sem, pr_sem, (seg_peers[m], lat)).start()
    total_count = jnp.sum(count.astype(f32), axis=1, keepdims=True)

    def tree(terms):
        w = 1
        while w < n_seg:
            terms = [terms[i] + terms[i + 1] for i in range(0, len(terms), 2)]
            w *= 2
        return terms[0]

    lat_cols, seg_cols = col_in.at[pl.ds(1, n_lat - 1)], col_in.at[pl.ds(n_lat + 1, n_seg - 1)]

    def seg_sum():
        remote(seg_cols, seg_cols, cs_sem, pr_sem, (seg_peers[1], lat)).wait_recv()
        psum[0] = tree([col_out[0]] + [col_in[n_lat + m] for m in range(1, n_seg)])
        for j in far_first:
            remote(psum.at[0], col_in.at[j], cs_sem, cr_sem, (seg, lat_peers[j])).start()

    for turn, turns in enumerate(ARRIVE):
        if turn == 2:
            pl.when(quarter >= 2)(seg_sum)
        elif turn == 3:
            pl.when(jnp.logical_not(quarter >= 2))(seg_sum)
        first, peers = order(turns) if turn else (0, lat_peers[:group])
        for i in range(group):
            j = first + i
            if turn or i:
                remote(
                    rows_out.at[j], rows_in.at[j], rs_sem, rr_sem.at[j - 1], (seg, peers[i])
                ).wait_recv()
                hand_on(rows_in.at[j], j, first // group, turn)

    theirs = gath.at[pl.ds(n_lat + 1, n_seg - 1)]
    remote(theirs, theirs, gs_sem, sr_sem, (seg_peers[1], lat)).wait_recv()
    slot_row = lax.broadcasted_iota(i32, (total_slots, points), 0)
    picks = []
    for m in range(n_seg):
        theirs = gath[n_lat + m, 0:1, :] if m else sid
        picks.append((slot_row == theirs).astype(f32).T.astype(bf16))
    peers = n_lat - 1 + n_seg - 1

    def sent(ref, sem):
        remote(ref, ref, sem, sr_sem, (seg_peers[1], lat)).wait_send()

    sent(gath.at[pl.ds(0, peers)], gs_sem)

    total = jnp.zeros((points, width), f32)
    for part_id in range(PARTS - 1):
        first, last = (part_id + 1 if part_id else 0) * group, (part_id + 2) * group
        theirs = far_rows.at[pl.ds(0, (n_seg - 1) * (last - first))]
        remote(theirs, theirs, rs_sem, xr_sem.at[part_id], (seg_peers[1], lat)).wait_recv()
        got = []
        mine = []
        for m in range(n_seg):
            mine.append(picks[m][:, first * slots : last * slots])
            for j in range(first, last):
                if m:
                    got.append(far_rows[m * n_lat + j])
                else:
                    got.append(rows_in[j] if j else rows_out[0])
        got = jnp.concatenate(got, axis=0)
        high = got.astype(bf16)
        rest = (got - high.astype(f32)).astype(bf16)
        total = total + jnp.dot(
            jnp.concatenate(mine + mine, axis=1),
            jnp.concatenate([high, rest], axis=0),
            preferred_element_type=f32,
        )
    stat = total / n_seg
    semi_ref[...] = stat.astype(semi_ref.dtype)
    remote(lat_cols, lat_cols, cs_sem, cr_sem, (seg, lat_peers[1])).wait_recv()
    col = psum[0]
    for j in range(1, n_lat):
        col = col + col_in[j]
    global_mean = (col / n_seg) / total_count
    row = lax.broadcasted_iota(i32, (block_size, width), 0)
    for b in range(blocks):
        block = stat[b * block_size : (b + 1) * block_size]
        block_sum = jnp.sum(jnp.where(row < cnt_ref[b], block, 0.0), axis=0, keepdims=True)
        mean = block_sum / jnp.full((1, width), cnt_ref[b], i32).astype(f32)
        excess_ref[b : b + 1, :] = mean - global_mean

    sent(col_in.at[pl.ds(0, peers)], cs_sem)
    for q in range(PARTS):
        skipped = group * sum(owner == q for owner, _ in DIRECT)
        across = group // 2 * sum(owner ^ g == q for owner, g in DIRECT)
        for core in range(2):

            @pl.when((quarter == q) & (parity == core))
            def _(skipped=skipped, across=across, core=core):
                count = n_seg * n_lat - 1 - (0 if core else skipped) + across
                sent(far_rows.at[pl.ds(0, count)], rs_sem)


def deliver(semi_ref, excess_ref, semi_out, excess_out, sem):
    copies = [
        pltpu.make_async_copy(semi_ref, semi_out, sem.at[0]),
        pltpu.make_async_copy(excess_ref, excess_out, sem.at[1]),
    ]
    for copy in copies:
        copy.start()
    for copy in copies:
        copy.wait()


def shards(n_lat, n_seg, coh_map, positions, counts):
    _, slice_bins, width = coh_map.shape
    points = positions.shape[1]
    blocks = counts.shape[0]
    slots = 2 * points // n_lat
    f32 = jnp.float32
    dma = pltpu.SemaphoreType.DMA
    made = pl.pallas_call(
        functools.partial(kernel, n_lat, n_seg),
        out_shape=(
            pltpu.VMEM((points, width), jnp.bfloat16),
            pltpu.VMEM((blocks, width), f32),
        ),
        in_specs=[
            pl.BlockSpec(memory_space=pl.ANY),
            pl.BlockSpec(memory_space=pl.ANY),
            pl.BlockSpec(memory_space=pl.ANY),
        ],
        out_specs=(
            pl.BlockSpec(memory_space=pltpu.VMEM),
            pl.BlockSpec(memory_space=pltpu.VMEM),
        ),
        scratch_shapes=[
            pltpu.VMEM((1, points), jnp.int32),
            pltpu.SMEM((blocks,), jnp.int32),
            pltpu.VMEM((slice_bins, width), coh_map.dtype),
            pltpu.VMEM((n_lat + n_seg, 4, points), jnp.int32),
            pltpu.VMEM((n_lat, slots, width), f32),
            pltpu.VMEM((n_lat, slots, width), f32),
            pltpu.VMEM((1, 1, width), f32),
            pltpu.VMEM((n_lat + n_seg, 1, width), f32),
            pltpu.VMEM((n_seg * n_lat + n_lat // PARTS, slots, width), f32),
            pltpu.VMEM((1, 1, width), f32),
            dma,
            dma,
            dma((PARTS,)),
            dma,
            dma((n_lat - 1,)),
            dma,
            dma,
            dma((PARTS - 1,)),
            dma,
            dma,
            dma((2,)),
        ],
        compiler_params=pltpu.CompilerParams(collective_id=0, has_side_effects=True),
    )(positions, counts, coh_map)
    made = [pltpu.with_memory_space_constraint(x, pltpu.VMEM) for x in made]
    return pl.pallas_call(
        deliver,
        out_shape=tuple(jax.ShapeDtypeStruct(x.shape, x.dtype) for x in made),
        in_specs=[pl.BlockSpec(memory_space=pltpu.VMEM)] * 2,
        out_specs=(pl.BlockSpec(memory_space=pl.ANY),) * 2,
        scratch_shapes=[dma((2,))],
    )(*made)


def solution(mesh):
    in_specs = (P("seg", "lat", None), P("seg", "lat"), P("lat"))
    out_specs = (P("lat", None), P("lat", None))
    body = functools.partial(shards, mesh.shape["lat"], mesh.shape["seg"])
    return jax.shard_map(body, mesh=mesh, in_specs=in_specs, out_specs=out_specs, check_vma=False)
```

```python
import functools

import jax
import jax.numpy as jnp
from jax import lax
from jax.experimental import pallas as pl
from jax.experimental.pallas import tpu as pltpu
from jax.sharding import PartitionSpec as P

MESH = pl.DeviceIdType.MESH
PARTS = 4
DIRECT = ((0, 1), (0, 3), (1, 2))
STEPS = (((0, 0, 0, 0),), ((1, 1, 2, 1),), ((2, 3, 1, 3), (3, 2, 3, 2)))
ARRIVE = ((0, 0, 0, 0), (1, 1, 1, 1), (2, 3, 3, 2), (3, 2, 2, 3))


def flip(index, mask):
    out = index
    w = 1
    while w <= mask:
        if mask & w:
            out = out + w - 2 * w * lax.rem(index // w, 2)
        w *= 2
    return out


def kernel(
    n_lat,
    n_seg,
    pos_hbm,
    cnt_hbm,
    coh_hbm,
    semi_ref,
    excess_ref,
    pos_ref,
    cnt_ref,
    coh,
    gath,
    rows_out,
    rows_in,
    col_out,
    col_in,
    far_rows,
    psum,
    coh_sem,
    gs_sem,
    gr_sem,
    rs_sem,
    rr_sem,
    cs_sem,
    cr_sem,
    xr_sem,
    sr_sem,
    pr_sem,
    in_sem,
):
    lat = lax.axis_index("lat")
    seg = lax.axis_index("seg")
    slice_bins, width = coh.shape
    points = pos_ref.shape[1]
    blocks = cnt_ref.shape[0]
    block_size = points // blocks
    slots = 2 * points // n_lat
    total_slots = n_lat * slots
    f32, bf16, i32 = jnp.float32, jnp.bfloat16, jnp.int32
    group = n_lat // PARTS
    quarter = lat // group
    parity = lax.rem(lat, 2)
    late = quarter // 3
    third = quarter // 2 - late
    second = quarter - 2 * third - 3 * late
    is_quarter = (1 - second - third - late, second, third, late)

    def remote(src, dst, send_sem, recv_sem, to):
        return pltpu.make_async_remote_copy(
            src_ref=src,
            dst_ref=dst,
            send_sem=send_sem,
            recv_sem=recv_sem,
            device_id=to,
            device_id_type=MESH,
        )

    barrier = pltpu.get_barrier_semaphore()
    lat_peers = [flip(lat, j) for j in range(n_lat)]
    seg_peers = [flip(seg, m) for m in range(n_seg)]
    far_first = list(range(n_lat - 1, 0, -1))
    seg_far_first = list(range(n_seg - 1, 0, -1))
    for j in far_first:
        pl.semaphore_signal(barrier, inc=1, device_id=(seg, lat_peers[j]), device_id_type=MESH)
    for m in seg_far_first:
        pl.semaphore_signal(barrier, inc=1, device_id=(seg_peers[m], lat), device_id_type=MESH)

    for owner, g in DIRECT:

        @pl.when((quarter == owner) & (parity == 0))
        def _(g=g):
            for j in range(g * group, (g + 1) * group):
                pl.semaphore_signal(
                    barrier, inc=1, device_id=(seg_peers[-1], lat_peers[j]), device_id_type=MESH
                )

    small = [
        pltpu.make_async_copy(pos_hbm, pos_ref, in_sem.at[0]),
        pltpu.make_async_copy(cnt_hbm, cnt_ref, in_sem.at[1]),
    ]
    for copy in small:
        copy.start()
    load = pltpu.make_async_copy(coh_hbm.at[0], coh, coh_sem)
    load.start()
    for copy in small:
        copy.wait()

    pos = pos_ref[...]
    lane = lax.broadcasted_iota(i32, (1, points), 1)
    dest = (pos // 256) // slice_bins
    rel = jnp.bitwise_xor(dest, jnp.full((1, points), lat, i32))
    hits = lax.broadcasted_iota(i32, (n_lat, points), 0) == rel
    hits_f = hits.astype(f32)
    tri = (
        lax.broadcasted_iota(i32, (points, points), 0)
        < lax.broadcasted_iota(i32, (points, points), 1)
    ).astype(f32)
    before = jnp.dot(hits_f.astype(bf16), tri.astype(bf16), preferred_element_type=f32)
    slot = jnp.sum(before * hits_f, axis=0, keepdims=True).astype(i32)
    sid = rel * slots + slot
    limit = jnp.zeros((1, points), i32)
    for b in range(blocks):
        limit = jnp.where(lane // block_size == b, cnt_ref[b], limit)
    valid = (lane % block_size < limit).astype(i32)
    gath[0, 0:1, :] = sid
    gath[0, 1:2, :] = pos
    gath[0, 2:3, :] = valid
    gath[0, 3:4, :] = valid

    straight = sum(is_quarter[owner ^ g] for owner, g in DIRECT)
    pl.semaphore_wait(barrier, n_lat - 1 + n_seg - 1 + straight * (group // 2))

    sends = {
        j: remote(gath.at[0], gath.at[j], gs_sem, gr_sem.at[j // group], (seg, lat_peers[j]))
        for j in far_first
    }
    for j in far_first:
        sends[j].start()
    sid_sends = [
        remote(gath.at[0], gath.at[n_lat + m], gs_sem, sr_sem, (seg_peers[m], lat))
        for m in seg_far_first
    ]
    for copy in sid_sends:
        copy.start()

    pos_bits = 8
    bin_bits = (slice_bins - 1).bit_length()
    depth = min(256, slice_bins)
    depth_bits = depth.bit_length() - 1
    base = lat * (slice_bins << pos_bits)
    flag = slice_bins << pos_bits
    sub = lax.broadcasted_iota(i32, (slots, points), 0)
    chunks = slice_bins // depth
    count = jnp.zeros((1, points), i32)
    col = jnp.zeros((1, width), f32)

    def mixed(plain, in_second, in_third, in_last):
        return (
            plain
            + second * (in_second - plain)
            + third * (in_third - plain)
            + late * (in_last - plain)
        )

    def order(turns):
        first = mixed(*turns) * group
        peers = [mixed(*(lat_peers[g * group + i] for g in turns)) for i in range(group)]
        return first, peers

    def hand_on(src, j, g, turn=0):
        for m in seg_far_first:
            copy = remote(
                src, far_rows.at[m * n_lat + j], rs_sem, xr_sem.at[g - (g + PARTS - 1) // PARTS], (seg_peers[m], lat)
            )
            skips = [owner for owner, r in DIRECT if ARRIVE[turn][owner] == r]
            if turn and skips and m == n_seg - 1:
                skip = sum(is_quarter[owner] for owner in skips) * (1 - parity)
                pl.when(skip == 0)(copy.start)
            else:
                copy.start()

    for step, turns in enumerate(STEPS):
        places = [order(t) if step else (0, lat_peers[:group]) for t in turns]
        cols = []
        for first, peers in places:
            rng = pl.ds(first, group) if step else pl.ds(1, group - 1)
            remote(
                gath.at[rng], gath.at[rng], gs_sem, gr_sem.at[first // group], (seg, peers[-1])
            ).wait_recv()
            for i in range(group):
                j = first + i
                live_row = gath[j, 2:3, :]
                code = (gath[j, 1:2, :] - base + flag * (1 + live_row)).astype(f32)
                here = (gath[j, 0:1, :] - j * slots) == sub
                cols.append(jnp.sum(jnp.where(here, code, 0.0), axis=1, keepdims=True))
                count = count + live_row
        code = jnp.concatenate(cols, axis=0).astype(i32)
        kind = lax.shift_right_logical(code, bin_bits + pos_bits)
        low = lax.shift_right_logical(code & (flag - 1), pos_bits)
        upper = (code & ((1 << pos_bits) - 1)).astype(f32) * (1.0 / (1 << pos_bits))
        chunk = jnp.where(kind > 0, lax.shift_right_logical(low, depth_bits), -2)
        in_chunk = low & (depth - 1)
        bins = lax.broadcasted_iota(i32, (code.shape[0], depth), 1)
        zero = jnp.zeros(bins.shape, bf16)
        local = jnp.where(bins == in_chunk, 1.0 - upper, 0.0)
        local = jnp.where(bins == ((in_chunk + 1) & (depth - 1)), upper, local).astype(bf16)
        where_id = jnp.where(bins < in_chunk, chunk + 1, chunk).astype(f32).astype(bf16)
        if step == 0:
            load.wait()
        weights = jnp.concatenate(
            [jnp.where(where_id == jnp.asarray(c, bf16), local, zero) for c in range(chunks)],
            axis=1,
        )
        held = jnp.dot(weights, coh[...], preferred_element_type=f32)
        posts, crosses = [], []
        for n, (first, peers) in enumerate(places):
            for i in range(group):
                at = (n * group + i) * slots
                rows_out[first + i] = held[at : at + slots, :]
            if step == 0:
                for j in range(1, group):
                    remote(
                        rows_out.at[j], rows_in.at[j], rs_sem, rr_sem.at[j - 1], (seg, lat_peers[j])
                    ).start()
                hand_on(rows_out.at[0], 0, 0)
                continue
            def post(odd, first=first, peers=peers):
                for i in range(odd, group, 2):
                    turn = parity if odd == 0 else -parity
                    j = first + i + turn
                    peer = peers[i] + parity * (peers[i ^ 1] - peers[i])
                    remote(
                        rows_out.at[j], rows_in.at[j], rs_sem, rr_sem.at[j - 1], (seg, peer)
                    ).start()

            def across(first=first, peers=peers):
                for i in range(0, group, 2):
                    j = first + i + parity
                    peer = peers[i] + parity * (peers[i + 1] - peers[i])
                    remote(
                        rows_out.at[j],
                        far_rows.at[(n_seg - 1) * n_lat + j],
                        rs_sem,
                        xr_sem.at[first // group - 1],
                        (seg_peers[-1], peer),
                    ).start()

            posts.append(post)
            crosses.append(across)
        for what, n in ((0, 0), (1, 0), (1, 1), (2, 0), (0, 1), (2, 1)) if step == 2 else ((0, 0), (1, 0), (2, 0)) if step else ():
            if what < 2:
                posts[n](what)
                continue
            makers = [owner ^ r for owner, r in DIRECT if turns[n][owner ^ r] == r]
            if makers:
                pl.when(sum(is_quarter[q] for q in makers) == 1)(crosses[n])
        if step == 1:
            remote(
                rows_out.at[1], rows_in.at[1], rs_sem, rr_sem.at[0], (seg, lat_peers[1])
            ).wait_recv()
            hand_on(rows_in.at[1], 1, 0)
        col = col + jnp.sum(jnp.where(kind > 1, held, 0.0), axis=0, keepdims=True)
    col_out[0] = col
    for m in seg_far_first:
        remote(col_out.at[0], col_in.at[n_lat + m], cs_sem, pr_sem, (seg_peers[m], lat)).start()
    total_count = jnp.sum(count.astype(f32), axis=1, keepdims=True)

    def tree(terms):
        w = 1
        while w < n_seg:
            terms = [terms[i] + terms[i + 1] for i in range(0, len(terms), 2)]
            w *= 2
        return terms[0]

    lat_cols, seg_cols = col_in.at[pl.ds(1, n_lat - 1)], col_in.at[pl.ds(n_lat + 1, n_seg - 1)]

    def seg_sum():
        remote(seg_cols, seg_cols, cs_sem, pr_sem, (seg_peers[1], lat)).wait_recv()
        psum[0] = tree([col_out[0]] + [col_in[n_lat + m] for m in range(1, n_seg)])
        for j in far_first:
            remote(psum.at[0], col_in.at[j], cs_sem, cr_sem, (seg, lat_peers[j])).start()

    for turn, turns in enumerate(ARRIVE):
        if turn == 2:
            pl.when(quarter >= 2)(seg_sum)
        elif turn == 3:
            pl.when(jnp.logical_not(quarter >= 2))(seg_sum)
        first, peers = order(turns) if turn else (0, lat_peers[:group])
        def one_by_one(turn=turn, first=first, peers=peers):
            for i in range(group):
                j = first + i
                if turn or i > 1:
                    remote(
                        rows_out.at[j], rows_in.at[j], rs_sem, rr_sem.at[j - 1], (seg, peers[i])
                    ).wait_recv()
                    hand_on(rows_in.at[j], j, first // group, turn)

        def together(turn=turn, first=first, peers=peers):
            for i in range(group):
                remote(
                    rows_out.at[0], rows_in.at[0], rs_sem, rr_sem.at[first + i - 1], (seg, peers[i])
                ).wait_recv()
            g = first // group
            for m in seg_far_first:
                copy = remote(
                    rows_in.at[pl.ds(first, group)],
                    far_rows.at[pl.ds(m * n_lat + first, group)],
                    rs_sem,
                    xr_sem.at[g - (g + PARTS - 1) // PARTS],
                    (seg_peers[m], lat),
                )
                skips = [owner for owner, r in DIRECT if ARRIVE[turn][owner] == r]
                if skips and m == n_seg - 1:
                    pl.when(sum(is_quarter[owner] for owner in skips) == 0)(copy.start)
                else:
                    copy.start()

        if turn in (2, 3):
            whole = (parity == 0) & (quarter == 0)
            pl.when(whole)(together)
            pl.when(jnp.logical_not(whole))(one_by_one)
        else:
            one_by_one()

    theirs = gath.at[pl.ds(n_lat + 1, n_seg - 1)]
    remote(theirs, theirs, gs_sem, sr_sem, (seg_peers[1], lat)).wait_recv()
    slot_row = lax.broadcasted_iota(i32, (total_slots, points), 0)
    picks = []
    for m in range(n_seg):
        theirs = gath[n_lat + m, 0:1, :] if m else sid
        picks.append((slot_row == theirs).astype(f32).T.astype(bf16))
    peers = n_lat - 1 + n_seg - 1

    def sent(ref, sem):
        remote(ref, ref, sem, sr_sem, (seg_peers[1], lat)).wait_send()

    sent(gath.at[pl.ds(0, peers)], gs_sem)

    total = jnp.zeros((points, width), f32)
    for part_id in range(PARTS - 1):
        first, last = (part_id + 1 if part_id else 0) * group, (part_id + 2) * group
        theirs = far_rows.at[pl.ds(0, (n_seg - 1) * (last - first))]
        remote(theirs, theirs, rs_sem, xr_sem.at[part_id], (seg_peers[1], lat)).wait_recv()
        got = []
        mine = []
        for m in range(n_seg):
            mine.append(picks[m][:, first * slots : last * slots])
            for j in range(first, last):
                if m:
                    got.append(far_rows[m * n_lat + j])
                else:
                    got.append(rows_in[j] if j else rows_out[0])
        got = jnp.concatenate(got, axis=0)
        high = got.astype(bf16)
        rest = (got - high.astype(f32)).astype(bf16)
        total = total + jnp.dot(
            jnp.concatenate(mine + mine, axis=1),
            jnp.concatenate([high, rest], axis=0),
            preferred_element_type=f32,
        )
    stat = total / n_seg
    semi_ref[...] = stat.astype(semi_ref.dtype)
    remote(lat_cols, lat_cols, cs_sem, cr_sem, (seg, lat_peers[1])).wait_recv()
    col = psum[0]
    for j in range(1, n_lat):
        col = col + col_in[j]
    global_mean = (col / n_seg) / total_count
    row = lax.broadcasted_iota(i32, (block_size, width), 0)
    for b in range(blocks):
        block = stat[b * block_size : (b + 1) * block_size]
        block_sum = jnp.sum(jnp.where(row < cnt_ref[b], block, 0.0), axis=0, keepdims=True)
        mean = block_sum / jnp.full((1, width), cnt_ref[b], i32).astype(f32)
        excess_ref[b : b + 1, :] = mean - global_mean

    sent(col_in.at[pl.ds(0, peers)], cs_sem)
    for q in range(PARTS):
        skipped = group * sum(owner == q for owner, _ in DIRECT)
        across = group // 2 * sum(owner ^ g == q for owner, g in DIRECT)
        for core in range(2):

            @pl.when((quarter == q) & (parity == core))
            def _(skipped=skipped, across=across, core=core):
                count = n_seg * n_lat - 1 - (0 if core else skipped) + across
                sent(far_rows.at[pl.ds(0, count)], rs_sem)


def deliver(semi_ref, excess_ref, semi_out, excess_out, sem):
    copies = [
        pltpu.make_async_copy(semi_ref, semi_out, sem.at[0]),
        pltpu.make_async_copy(excess_ref, excess_out, sem.at[1]),
    ]
    for copy in copies:
        copy.start()
    for copy in copies:
        copy.wait()


def shards(n_lat, n_seg, coh_map, positions, counts):
    _, slice_bins, width = coh_map.shape
    points = positions.shape[1]
    blocks = counts.shape[0]
    slots = 2 * points // n_lat
    f32 = jnp.float32
    dma = pltpu.SemaphoreType.DMA
    made = pl.pallas_call(
        functools.partial(kernel, n_lat, n_seg),
        out_shape=(
            pltpu.VMEM((points, width), jnp.bfloat16),
            pltpu.VMEM((blocks, width), f32),
        ),
        in_specs=[
            pl.BlockSpec(memory_space=pl.ANY),
            pl.BlockSpec(memory_space=pl.ANY),
            pl.BlockSpec(memory_space=pl.ANY),
        ],
        out_specs=(
            pl.BlockSpec(memory_space=pltpu.VMEM),
            pl.BlockSpec(memory_space=pltpu.VMEM),
        ),
        scratch_shapes=[
            pltpu.VMEM((1, points), jnp.int32),
            pltpu.SMEM((blocks,), jnp.int32),
            pltpu.VMEM((slice_bins, width), coh_map.dtype),
            pltpu.VMEM((n_lat + n_seg, 4, points), jnp.int32),
            pltpu.VMEM((n_lat, slots, width), f32),
            pltpu.VMEM((n_lat, slots, width), f32),
            pltpu.VMEM((1, 1, width), f32),
            pltpu.VMEM((n_lat + n_seg, 1, width), f32),
            pltpu.VMEM((n_seg * n_lat + n_lat // PARTS, slots, width), f32),
            pltpu.VMEM((1, 1, width), f32),
            dma,
            dma,
            dma((PARTS,)),
            dma,
            dma((n_lat - 1,)),
            dma,
            dma,
            dma((PARTS - 1,)),
            dma,
            dma,
            dma((2,)),
        ],
        compiler_params=pltpu.CompilerParams(collective_id=0, has_side_effects=True),
    )(positions, counts, coh_map)
    made = [pltpu.with_memory_space_constraint(x, pltpu.VMEM) for x in made]
    return pl.pallas_call(
        deliver,
        out_shape=tuple(jax.ShapeDtypeStruct(x.shape, x.dtype) for x in made),
        in_specs=[pl.BlockSpec(memory_space=pltpu.VMEM)] * 2,
        out_specs=(pl.BlockSpec(memory_space=pl.ANY),) * 2,
        scratch_shapes=[dma((2,))],
    )(*made)


def solution(mesh):
    in_specs = (P("seg", "lat", None), P("seg", "lat"), P("lat"))
    out_specs = (P("lat", None), P("lat", None))
    body = functools.partial(shards, mesh.shape["lat"], mesh.shape["seg"])
    return jax.shard_map(body, mesh=mesh, in_specs=in_specs, out_specs=out_specs, check_vma=False)
```

```python
import functools

import jax
import jax.numpy as jnp
from jax import lax
from jax.experimental import pallas as pl
from jax.experimental.pallas import tpu as pltpu
from jax.sharding import PartitionSpec as P

MESH = pl.DeviceIdType.MESH
PARTS = 4
DIRECT = ((0, 1), (0, 3), (1, 2))
STEPS = (((0, 0, 0, 0),), ((1, 1, 2, 1),), ((2, 3, 1, 3), (3, 2, 3, 2)))
ARRIVE = ((0, 0, 0, 0), (1, 1, 1, 1), (2, 3, 3, 2), (3, 2, 2, 3))


def flip(index, mask):
    out = index
    w = 1
    while w <= mask:
        if mask & w:
            out = out + w - 2 * w * lax.rem(index // w, 2)
        w *= 2
    return out


def kernel(
    n_lat,
    n_seg,
    pos_hbm,
    cnt_hbm,
    coh_hbm,
    semi_ref,
    excess_ref,
    pos_ref,
    cnt_ref,
    coh,
    gath,
    rows_out,
    rows_in,
    col_out,
    col_in,
    far_rows,
    psum,
    coh_sem,
    gs_sem,
    gr_sem,
    rs_sem,
    rr_sem,
    cs_sem,
    cr_sem,
    xr_sem,
    sr_sem,
    pr_sem,
    in_sem,
):
    lat = lax.axis_index("lat")
    seg = lax.axis_index("seg")
    slice_bins, width = coh.shape
    points = pos_ref.shape[1]
    blocks = cnt_ref.shape[0]
    block_size = points // blocks
    slots = 2 * points // n_lat
    total_slots = n_lat * slots
    f32, bf16, i32 = jnp.float32, jnp.bfloat16, jnp.int32
    group = n_lat // PARTS
    quarter = lat // group
    parity = lax.rem(lat, 2)
    late = quarter // 3
    third = quarter // 2 - late
    second = quarter - 2 * third - 3 * late
    is_quarter = (1 - second - third - late, second, third, late)

    def remote(src, dst, send_sem, recv_sem, to):
        return pltpu.make_async_remote_copy(
            src_ref=src,
            dst_ref=dst,
            send_sem=send_sem,
            recv_sem=recv_sem,
            device_id=to,
            device_id_type=MESH,
        )

    barrier = pltpu.get_barrier_semaphore()
    lat_peers = [flip(lat, j) for j in range(n_lat)]
    seg_peers = [flip(seg, m) for m in range(n_seg)]
    far_first = list(range(n_lat - 1, 0, -1))
    seg_far_first = list(range(n_seg - 1, 0, -1))
    for j in far_first:
        pl.semaphore_signal(barrier, inc=1, device_id=(seg, lat_peers[j]), device_id_type=MESH)
    for m in seg_far_first:
        pl.semaphore_signal(barrier, inc=1, device_id=(seg_peers[m], lat), device_id_type=MESH)

    for owner, g in DIRECT:

        @pl.when((quarter == owner) & (parity == 0))
        def _(g=g):
            for j in range(g * group, (g + 1) * group):
                pl.semaphore_signal(
                    barrier, inc=1, device_id=(seg_peers[-1], lat_peers[j]), device_id_type=MESH
                )

    small = [
        pltpu.make_async_copy(pos_hbm, pos_ref, in_sem.at[0]),
        pltpu.make_async_copy(cnt_hbm, cnt_ref, in_sem.at[1]),
    ]
    for copy in small:
        copy.start()
    load = pltpu.make_async_copy(coh_hbm.at[0], coh, coh_sem)
    load.start()
    for copy in small:
        copy.wait()

    pos = pos_ref[...]
    lane = lax.broadcasted_iota(i32, (1, points), 1)
    dest = (pos // 256) // slice_bins
    rel = jnp.bitwise_xor(dest, jnp.full((1, points), lat, i32))
    hits = lax.broadcasted_iota(i32, (n_lat, points), 0) == rel
    hits_f = hits.astype(f32)
    tri = (
        lax.broadcasted_iota(i32, (points, points), 0)
        < lax.broadcasted_iota(i32, (points, points), 1)
    ).astype(f32)
    before = jnp.dot(hits_f.astype(bf16), tri.astype(bf16), preferred_element_type=f32)
    slot = jnp.sum(before * hits_f, axis=0, keepdims=True).astype(i32)
    sid = rel * slots + slot
    limit = jnp.zeros((1, points), i32)
    for b in range(blocks):
        limit = jnp.where(lane // block_size == b, cnt_ref[b], limit)
    valid = (lane % block_size < limit).astype(i32)
    gath[0, 0:1, :] = sid
    gath[0, 1:2, :] = pos
    gath[0, 2:3, :] = valid

    straight = sum(is_quarter[owner ^ g] for owner, g in DIRECT)
    pl.semaphore_wait(barrier, n_lat - 1 + n_seg - 1 + straight * (group // 2))

    sends = {
        j: remote(gath.at[0], gath.at[j], gs_sem, gr_sem.at[j // group], (seg, lat_peers[j]))
        for j in far_first
    }
    for j in far_first:
        sends[j].start()
    sid_sends = [
        remote(gath.at[0], gath.at[n_lat + m], gs_sem, sr_sem, (seg_peers[m], lat))
        for m in seg_far_first
    ]
    for copy in sid_sends:
        copy.start()

    pos_bits = 8
    bin_bits = (slice_bins - 1).bit_length()
    depth = min(256, slice_bins)
    depth_bits = depth.bit_length() - 1
    base = lat * (slice_bins << pos_bits)
    flag = slice_bins << pos_bits
    sub = lax.broadcasted_iota(i32, (slots, points), 0)
    chunks = slice_bins // depth
    count = jnp.zeros((1, points), i32)
    col = jnp.zeros((1, width), f32)

    def mixed(plain, in_second, in_third, in_last):
        return (
            plain
            + second * (in_second - plain)
            + third * (in_third - plain)
            + late * (in_last - plain)
        )

    def order(turns):
        first = mixed(*turns) * group
        peers = [mixed(*(lat_peers[g * group + i] for g in turns)) for i in range(group)]
        return first, peers

    def hand_on(src, j, g, turn=0):
        for m in seg_far_first:
            copy = remote(
                src, far_rows.at[m * n_lat + j], rs_sem, xr_sem.at[g - (g + PARTS - 1) // PARTS], (seg_peers[m], lat)
            )
            skips = [owner for owner, r in DIRECT if ARRIVE[turn][owner] == r]
            if turn and skips and m == n_seg - 1:
                skip = sum(is_quarter[owner] for owner in skips) * (1 - parity)
                pl.when(skip == 0)(copy.start)
            else:
                copy.start()

    for step, turns in enumerate(STEPS):
        places = [order(t) if step else (0, lat_peers[:group]) for t in turns]
        cols = []
        for first, peers in places:
            rng = pl.ds(first, group) if step else pl.ds(1, group - 1)
            remote(
                gath.at[rng], gath.at[rng], gs_sem, gr_sem.at[first // group], (seg, peers[-1])
            ).wait_recv()
            for i in range(group):
                j = first + i
                live_row = gath[j, 2:3, :]
                code = (gath[j, 1:2, :] - base + flag * (1 + live_row)).astype(f32)
                here = (gath[j, 0:1, :] - j * slots) == sub
                cols.append(jnp.sum(jnp.where(here, code, 0.0), axis=1, keepdims=True))
                count = count + live_row
        code = jnp.concatenate(cols, axis=0).astype(i32)
        kind = lax.shift_right_logical(code, bin_bits + pos_bits)
        low = lax.shift_right_logical(code & (flag - 1), pos_bits)
        upper = (code & ((1 << pos_bits) - 1)).astype(f32) * (1.0 / (1 << pos_bits))
        chunk = jnp.where(kind > 0, lax.shift_right_logical(low, depth_bits), -2)
        in_chunk = low & (depth - 1)
        bins = lax.broadcasted_iota(i32, (code.shape[0], depth), 1)
        zero = jnp.zeros(bins.shape, bf16)
        local = jnp.where(bins == in_chunk, 1.0 - upper, 0.0)
        local = jnp.where(bins == ((in_chunk + 1) & (depth - 1)), upper, local).astype(bf16)
        where_id = jnp.where(bins < in_chunk, chunk + 1, chunk).astype(f32).astype(bf16)
        if step == 0:
            load.wait()
        weights = jnp.concatenate(
            [jnp.where(where_id == jnp.asarray(c, bf16), local, zero) for c in range(chunks)],
            axis=1,
        )
        held = jnp.dot(weights, coh[...], preferred_element_type=f32)
        posts, crosses = [], []
        for n, (first, peers) in enumerate(places):
            for i in range(group):
                at = (n * group + i) * slots
                rows_out[first + i] = held[at : at + slots, :]
            if step == 0:
                for j in range(1, group):
                    remote(
                        rows_out.at[j], rows_in.at[j], rs_sem, rr_sem.at[j - 1], (seg, lat_peers[j])
                    ).start()
                hand_on(rows_out.at[0], 0, 0)
                continue
            def post(odd, first=first, peers=peers):
                for i in range(odd, group, 2):
                    turn = parity if odd == 0 else -parity
                    j = first + i + turn
                    peer = peers[i] + parity * (peers[i ^ 1] - peers[i])
                    remote(
                        rows_out.at[j], rows_in.at[j], rs_sem, rr_sem.at[j - 1], (seg, peer)
                    ).start()

            def across(first=first, peers=peers):
                for i in range(0, group, 2):
                    j = first + i + parity
                    peer = peers[i] + parity * (peers[i + 1] - peers[i])
                    remote(
                        rows_out.at[j],
                        far_rows.at[(n_seg - 1) * n_lat + j],
                        rs_sem,
                        xr_sem.at[first // group - 1],
                        (seg_peers[-1], peer),
                    ).start()

            posts.append(post)
            crosses.append(across)
        for what, n in ((0, 0), (1, 0), (1, 1), (2, 0), (0, 1), (2, 1)) if step == 2 else ((0, 0), (1, 0), (2, 0)) if step else ():
            if what < 2:
                posts[n](what)
                continue
            makers = [owner ^ r for owner, r in DIRECT if turns[n][owner ^ r] == r]
            if makers:
                pl.when(sum(is_quarter[q] for q in makers) == 1)(crosses[n])
        if step == 1:
            remote(
                rows_out.at[1], rows_in.at[1], rs_sem, rr_sem.at[0], (seg, lat_peers[1])
            ).wait_recv()
            hand_on(rows_in.at[1], 1, 0)
        col = col + jnp.sum(jnp.where(kind > 1, held, 0.0), axis=0, keepdims=True)
    col_out[0] = col
    for m in seg_far_first:
        remote(col_out.at[0], col_in.at[n_lat + m], cs_sem, pr_sem, (seg_peers[m], lat)).start()
    total_count = jnp.sum(count.astype(f32), axis=1, keepdims=True)

    def tree(terms):
        w = 1
        while w < n_seg:
            terms = [terms[i] + terms[i + 1] for i in range(0, len(terms), 2)]
            w *= 2
        return terms[0]

    lat_cols, seg_cols = col_in.at[pl.ds(1, n_lat - 1)], col_in.at[pl.ds(n_lat + 1, n_seg - 1)]

    def seg_sum():
        remote(seg_cols, seg_cols, cs_sem, pr_sem, (seg_peers[1], lat)).wait_recv()
        psum[0] = tree([col_out[0]] + [col_in[n_lat + m] for m in range(1, n_seg)])
        for j in far_first:
            remote(psum.at[0], col_in.at[j], cs_sem, cr_sem, (seg, lat_peers[j])).start()

    for turn, turns in enumerate(ARRIVE):
        if turn == 2:
            pl.when(quarter >= 2)(seg_sum)
        elif turn == 3:
            pl.when(jnp.logical_not(quarter >= 2))(seg_sum)
        first, peers = order(turns) if turn else (0, lat_peers[:group])
        def one_by_one(turn=turn, first=first, peers=peers):
            for i in range(group):
                j = first + i
                if turn or i > 1:
                    remote(
                        rows_out.at[j], rows_in.at[j], rs_sem, rr_sem.at[j - 1], (seg, peers[i])
                    ).wait_recv()
                    hand_on(rows_in.at[j], j, first // group, turn)

        def together(turn=turn, first=first, peers=peers):
            for i in range(group):
                remote(
                    rows_out.at[0], rows_in.at[0], rs_sem, rr_sem.at[first + i - 1], (seg, peers[i])
                ).wait_recv()
            g = first // group
            for m in seg_far_first:
                copy = remote(
                    rows_in.at[pl.ds(first, group)],
                    far_rows.at[pl.ds(m * n_lat + first, group)],
                    rs_sem,
                    xr_sem.at[g - (g + PARTS - 1) // PARTS],
                    (seg_peers[m], lat),
                )
                skips = [owner for owner, r in DIRECT if ARRIVE[turn][owner] == r]
                if skips and m == n_seg - 1:
                    pl.when(sum(is_quarter[owner] for owner in skips) == 0)(copy.start)
                else:
                    copy.start()

        if turn in (2, 3):
            whole = (parity == 0) & (quarter == 0)
            pl.when(whole)(together)
            pl.when(jnp.logical_not(whole))(one_by_one)
        else:
            one_by_one()

    theirs = gath.at[pl.ds(n_lat + 1, n_seg - 1)]
    remote(theirs, theirs, gs_sem, sr_sem, (seg_peers[1], lat)).wait_recv()
    slot_row = lax.broadcasted_iota(i32, (total_slots, points), 0)
    picks = []
    for m in range(n_seg):
        theirs = gath[n_lat + m, 0:1, :] if m else sid
        picks.append((slot_row == theirs).astype(f32).T.astype(bf16))
    peers = n_lat - 1 + n_seg - 1

    def sent(ref, sem):
        remote(ref, ref, sem, sr_sem, (seg_peers[1], lat)).wait_send()

    sent(gath.at[pl.ds(0, peers)], gs_sem)

    total = jnp.zeros((points, width), f32)
    for part_id in range(PARTS - 1):
        first, last = (part_id + 1 if part_id else 0) * group, (part_id + 2) * group
        theirs = far_rows.at[pl.ds(0, (n_seg - 1) * (last - first))]
        remote(theirs, theirs, rs_sem, xr_sem.at[part_id], (seg_peers[1], lat)).wait_recv()
        got = []
        mine = []
        for m in range(n_seg):
            mine.append(picks[m][:, first * slots : last * slots])
            for j in range(first, last):
                if m:
                    got.append(far_rows[m * n_lat + j])
                else:
                    got.append(rows_in[j] if j else rows_out[0])
        got = jnp.concatenate(got, axis=0)
        high = got.astype(bf16)
        rest = (got - high.astype(f32)).astype(bf16)
        total = total + jnp.dot(
            jnp.concatenate(mine + mine, axis=1),
            jnp.concatenate([high, rest], axis=0),
            preferred_element_type=f32,
        )
    stat = total / n_seg
    semi_ref[...] = stat.astype(semi_ref.dtype)
    remote(lat_cols, lat_cols, cs_sem, cr_sem, (seg, lat_peers[1])).wait_recv()
    col = psum[0]
    for j in range(1, n_lat):
        col = col + col_in[j]
    global_mean = (col / n_seg) / total_count
    row = lax.broadcasted_iota(i32, (block_size, width), 0)
    for b in range(blocks):
        block = stat[b * block_size : (b + 1) * block_size]
        block_sum = jnp.sum(jnp.where(row < cnt_ref[b], block, 0.0), axis=0, keepdims=True)
        mean = block_sum / jnp.full((1, width), cnt_ref[b], i32).astype(f32)
        excess_ref[b : b + 1, :] = mean - global_mean

    sent(col_in.at[pl.ds(0, peers)], cs_sem)
    for q in range(PARTS):
        skipped = group * sum(owner == q for owner, _ in DIRECT)
        across = group // 2 * sum(owner ^ g == q for owner, g in DIRECT)
        for core in range(2):

            @pl.when((quarter == q) & (parity == core))
            def _(skipped=skipped, across=across, core=core):
                count = n_seg * n_lat - 1 - (0 if core else skipped) + across
                sent(far_rows.at[pl.ds(0, count)], rs_sem)


def deliver(semi_ref, excess_ref, semi_out, excess_out, sem):
    copies = [
        pltpu.make_async_copy(semi_ref, semi_out, sem.at[0]),
        pltpu.make_async_copy(excess_ref, excess_out, sem.at[1]),
    ]
    for copy in copies:
        copy.start()
    for copy in copies:
        copy.wait()


def shards(n_lat, n_seg, coh_map, positions, counts):
    _, slice_bins, width = coh_map.shape
    points = positions.shape[1]
    blocks = counts.shape[0]
    slots = 2 * points // n_lat
    f32 = jnp.float32
    dma = pltpu.SemaphoreType.DMA
    made = pl.pallas_call(
        functools.partial(kernel, n_lat, n_seg),
        out_shape=(
            pltpu.VMEM((points, width), jnp.bfloat16),
            pltpu.VMEM((blocks, width), f32),
        ),
        in_specs=[
            pl.BlockSpec(memory_space=pl.ANY),
            pl.BlockSpec(memory_space=pl.ANY),
            pl.BlockSpec(memory_space=pl.ANY),
        ],
        out_specs=(
            pl.BlockSpec(memory_space=pltpu.VMEM),
            pl.BlockSpec(memory_space=pltpu.VMEM),
        ),
        scratch_shapes=[
            pltpu.VMEM((1, points), jnp.int32),
            pltpu.SMEM((blocks,), jnp.int32),
            pltpu.VMEM((slice_bins, width), coh_map.dtype),
            pltpu.VMEM((n_lat + n_seg, 3, points), jnp.int32),
            pltpu.VMEM((n_lat, slots, width), f32),
            pltpu.VMEM((n_lat, slots, width), f32),
            pltpu.VMEM((1, 1, width), f32),
            pltpu.VMEM((n_lat + n_seg, 1, width), f32),
            pltpu.VMEM((n_seg * n_lat + n_lat // PARTS, slots, width), f32),
            pltpu.VMEM((1, 1, width), f32),
            dma,
            dma,
            dma((PARTS,)),
            dma,
            dma((n_lat - 1,)),
            dma,
            dma,
            dma((PARTS - 1,)),
            dma,
            dma,
            dma((2,)),
        ],
        compiler_params=pltpu.CompilerParams(collective_id=0, has_side_effects=True),
    )(positions, counts, coh_map)
    made = [pltpu.with_memory_space_constraint(x, pltpu.VMEM) for x in made]
    return pl.pallas_call(
        deliver,
        out_shape=tuple(jax.ShapeDtypeStruct(x.shape, x.dtype) for x in made),
        in_specs=[pl.BlockSpec(memory_space=pltpu.VMEM)] * 2,
        out_specs=(pl.BlockSpec(memory_space=pl.ANY),) * 2,
        scratch_shapes=[dma((2,))],
    )(*made)


def solution(mesh):
    in_specs = (P("seg", "lat", None), P("seg", "lat"), P("lat"))
    out_specs = (P("lat", None), P("lat", None))
    body = functools.partial(shards, mesh.shape["lat"], mesh.shape["seg"])
    return jax.shard_map(body, mesh=mesh, in_specs=in_specs, out_specs=out_specs, check_vma=False)
```
